32 devices in a mesh: row: 4 (over z), col: 8 (over y, x, core).
Axes of the slice: x: 2, y: 2, z: 4, core: 2. Of those that a mesh axis runs over, the one named last changes fastest.
Arguments:
- layer_in: bfloat16 [2, 4096, 2048], P(None, ('row', 'col')), may hold values from -6 to 6
- earlier_outs: bfloat16 [4, 2, 4096, 2048], P(None, None, ('row', 'col')), may hold values from -6 to 6
- cotangent: bfloat16 [2, 4096, 2048], P(None, ('row', 'col')), may hold values from -6 to 6
- segments: int32 [2, 4096], P(None, 'row'), may hold values from 0 to 4095, as said below
- positions: int32 [2, 4096], P(None, 'row'), may hold values from 0 to 2044, as said below
- w_qkv: bfloat16 [3, 2048, 2048], P(None, 'row', 'col'), may hold values from -0.125 to 0.125
- w_out: bfloat16 [2048, 2048], P('col', 'row'), may hold values from -0.5 to 0.5
- w_up: bfloat16 [2048, 8192], P('row', 'col'), may hold values from -0.125 to 0.125
- w_down: bfloat16 [8192, 2048], P('col', 'row'), may hold values from -0.0625 to 0.0625
- ln_gains: bfloat16 [2, 2048], P(None, 'row'), may hold values from 0.25 to 1.75
- ln_biases: bfloat16 [2, 2048], P(None, 'row'), may hold values from -1.5 to 1.5
- dwa_weights: float32 [5], replicated, may hold values from 0.3 to 1
Outputs:
- out: bfloat16 [2, 4096, 2048], P(None, ('row', 'col'))
- grad_in: float32 [2, 4096, 2048], P(None, ('row', 'col'))
- grad_earlier: float32 [4, 2, 4096, 2048], P(None, None, ('row', 'col'))
- grad_w_qkv: float32 [3, 2048, 2048], P(None, 'row', 'col')
- grad_w_out: float32 [2048, 2048], P('col', 'row')
- grad_w_up: float32 [2048, 8192], P('row', 'col')
- grad_w_down: float32 [8192, 2048], P('col', 'row')
- grad_gains: float32 [2, 2048], P(None, 'row')
- grad_biases: float32 [2, 2048], P(None, 'row')
- grad_dwa: float32 [5], replicated
The draws below stay inside these ranges and needn't reach their ends.
Inputs may be any that keep to these rules, and one draw needn't show every extreme that they name: `segments`: each aligned run of 1024 tokens of a micro-batch is a sequence whose first and last tokens start documents; a token's number is the index, within its micro-batch, of the first token of its document, so numbers never fall within a sequence. `positions`: 0 at the first token of each document, rising by 1 or 2 from one token to the next within it.
All inputs are finite; a program needn't handle non-finite values.
Results may differ from the reference program's by a relative error of at most 0.014.
Values may be sent and summed in bfloat16 or wider, within the bound.
No kernel may reach another device: no remote copies, remote signals or barrier semaphores. Data moves between devices by JAX's collectives and lax.ppermute only.
A program may use at most 448 MiB of HBM per device.

```python
import jax
import jax.numpy as jnp
from jax import lax

D = 2048
HEADS = 32
HEAD = 64
FF = 8192
MICRO = 2
PRIOR = 4
LEN = 1024
HD = 2048
TOKENS = 4096


def doc_layout(key):
    doc_key = jax.random.fold_in(key, 977)
    rate_key, cut_key, step_key = jax.random.split(doc_key, 3)
    seq_count = MICRO * TOKENS // LEN
    levels = jax.random.randint(rate_key, (seq_count, 1), 1, 6, dtype=jnp.int32)
    span_sizes = jnp.power(jnp.int32(4), levels)
    cut_draws = jax.random.randint(cut_key, (seq_count, LEN), 0, 1 << 20, dtype=jnp.int32)
    pos_index = jnp.arange(LEN, dtype=jnp.int32)[None, :]
    edges = (pos_index == 0) | (pos_index == LEN - 1)
    first_seq = jnp.arange(seq_count, dtype=jnp.int32)[:, None] == 0
    boundary = (cut_draws % span_sizes == 0) | edges
    boundary = jnp.where(first_seq, edges, boundary)
    token_index = (jnp.arange(seq_count * LEN, dtype=jnp.int32) % TOKENS).reshape(seq_count, LEN)
    seg_ids = lax.cummax(jnp.where(boundary, token_index, 0), axis=1)
    step_sizes = jax.random.randint(step_key, (seq_count, LEN), 1, 3, dtype=jnp.int32)
    step_sizes = jnp.where(first_seq, jnp.int32(2), step_sizes)
    running = jnp.cumsum(step_sizes, axis=1, dtype=jnp.int32)
    places = running - lax.cummax(jnp.where(boundary, running, 0), axis=1)
    return (seg_ids.reshape(MICRO, TOKENS), places.reshape(MICRO, TOKENS))


def draw_segments(key, part):
    return doc_layout(key)[0]


def draw_positions(key, part):
    return doc_layout(key)[1]


def shard_levels(key, shape, shards, smallest, top_value):
    loudness = 1.0
    for position, parts in shards:
        draws = jax.random.uniform(jax.random.fold_in(jax.random.fold_in(key, 6), position), (parts,), jnp.float32, smallest / len(shards), top_value / len(shards))
        loudness = loudness * jnp.repeat(jnp.exp(draws), shape[position] // parts).reshape((-1,) + (1,) * (len(shape) - 1 - position))
    return loudness


def noise(own_key, dims, width, most, cuts=(), kind=jnp.bfloat16):
    loudness = shard_levels(own_key, dims, cuts, -0.22, 0.18) if cuts else 1.0
    values = jax.random.normal(own_key, dims, jnp.float32) * width * loudness
    return jnp.minimum(jnp.maximum(values, -most), most).astype(kind)


def setup_inputs(seed: int = 0) -> dict:
    key_list = jax.random.split(jax.random.key(seed), 13)
    return {
        "layer_in": noise(key_list[0], (MICRO, TOKENS, D), 1.0, 6.0, ((1, 32),)),
        "earlier_outs": noise(key_list[1], (PRIOR, MICRO, TOKENS, D), 1.0, 6.0, ((2, 32),)),
        "cotangent": noise(key_list[2], (MICRO, TOKENS, D), 1.0, 6.0, ((1, 32),)),
        "segments": draw_segments(jax.random.fold_in(key_list[12], 71), 0),
        "positions": draw_positions(jax.random.fold_in(key_list[12], 71), 0),
        "w_qkv": noise(key_list[5], (3, D, HD), D ** -0.5, 0.125, ((1, 4), (2, 8))),
        "w_out": noise(key_list[6], (HD, D), (HD // 16) ** -0.5, 0.5, ((0, 8), (1, 4))),
        "w_up": noise(key_list[7], (D, FF), D ** -0.5, 0.125, ((0, 4), (1, 8))),
        "w_down": noise(key_list[8], (FF, D), FF ** -0.5, 0.0625, ((0, 8), (1, 4))),
        "ln_gains": jnp.clip(1.0 + 0.15 * jax.random.normal(key_list[9], (2, D), jnp.float32), 0.25, 1.75).astype(jnp.bfloat16),
        "ln_biases": noise(key_list[10], (2, D), 0.3, 1.5, ((1, 4),)),
        "dwa_weights": jnp.clip(jax.random.uniform(key_list[11], (PRIOR + 1,), jnp.float32, 0.3, 1.0), 0.3, 1.0),
    }


@jax.custom_vjp
def low(v):
    return lax.optimization_barrier(v.astype(jnp.bfloat16)).astype(jnp.float32)

@jax.custom_vjp
def low_back(v):
    return v

def low_keep(v):
    return (low(v), None)

def low_pass(kept, grad):
    return (grad,)

def back_keep(v):
    return (v, None)

def back_low(kept, grad):
    return (low(grad),)
low.defvjp(low_keep, low_pass)
low_back.defvjp(back_keep, back_low)
EPSILON = 1e-05
NEG_FILL = -1e+30
HIGH = lax.Precision.HIGHEST

def normalize(values, ln_gain, ln_bias):
    centre = values - lax.optimization_barrier(jnp.mean(values, axis=-1, keepdims=True))
    return centre * lax.rsqrt(lax.optimization_barrier(jnp.mean(centre * centre, axis=-1, keepdims=True)) + EPSILON) * ln_gain + ln_bias

def rotate(values, places):
    half_size = HEAD // 2
    inverse = 10000.0 ** (-(jnp.arange(half_size, dtype=jnp.float32) * 2.0) / HEAD)
    angles = places.astype(jnp.float32)[:, None] * inverse[None, :]
    cos_part = jnp.cos(angles)[:, None, :]
    sin_part = jnp.sin(angles)[:, None, :]
    lead_half = values[..., :half_size]
    tail_half = values[..., half_size:]
    return jnp.concatenate([lead_half * cos_part - tail_half * sin_part, tail_half * cos_part + lead_half * sin_part], axis=-1)

def attend(packed):
    queries, key_vecs, val_vecs, seg_ids = packed
    pos_index = jnp.arange(LEN)
    doc_mask = (seg_ids[:, None] == seg_ids[None, :]) & (pos_index[None, :] <= pos_index[:, None])
    raw = jnp.einsum('qhe,khe->hqk', queries, key_vecs, precision=HIGH) * HEAD ** (-0.5)
    scores = jnp.where(doc_mask[None], low_back(raw), NEG_FILL)
    weights = low(jax.nn.softmax(scores, axis=-1))
    return jnp.einsum('hqk,khe->qhe', weights, val_vecs, precision=HIGH)

def block(resid_in, earlier, seg_ids, places, w_qkv, w_out, w_up, w_down, ln_gain, ln_bias, dwa_mix):
    head_shape = (TOKENS, HEADS, HEAD)
    seq_shape = (TOKENS // LEN, LEN, HEADS, HEAD)
    normed1 = low(normalize(resid_in, ln_gain[0], ln_bias[0]))
    qkv_proj = jnp.einsum('sd,jdh->jsh', normed1, w_qkv, precision=HIGH)
    queries = low(rotate(low_back(qkv_proj[0]).reshape(head_shape), places))
    key_vecs = low(rotate(low_back(qkv_proj[1]).reshape(head_shape), places))
    val_vecs = low(low_back(qkv_proj[2])).reshape(head_shape)
    attended = lax.map(jax.checkpoint(attend), (queries.reshape(seq_shape), key_vecs.reshape(seq_shape), val_vecs.reshape(seq_shape), seg_ids.reshape(TOKENS // LEN, LEN)))
    attended = low(low_back(attended.reshape(TOKENS, HD)))
    resid = resid_in + low_back(jnp.dot(attended, w_out, precision=HIGH))
    normed2 = low(normalize(resid, ln_gain[1], ln_bias[1]))
    pre_act = low_back(jnp.dot(normed2, w_up, precision=HIGH))
    hidden = low(jax.nn.gelu(pre_act, approximate=False))
    block_out = resid + low_back(jnp.dot(hidden, w_down, precision=HIGH))
    mix_sum = dwa_mix[0] * earlier[0]
    for level in range(1, PRIOR):
        mix_sum = mix_sum + dwa_mix[level] * earlier[level]
    return mix_sum + dwa_mix[PRIOR] * block_out

def forward(layer_in, earlier_outs, w_qkv, w_out, w_up, w_down, ln_gain, ln_bias, dwa_mix, segments, positions):

    def micro_step(carry, packed):
        resid_in, earlier, seg_ids, places = packed
        return (carry, block(resid_in, earlier, seg_ids, places, w_qkv, w_out, w_up, w_down, ln_gain, ln_bias, dwa_mix))
    earlier_first = jnp.moveaxis(earlier_outs, 1, 0)
    unused, outputs = lax.scan(micro_step, jnp.zeros((), jnp.float32), (layer_in, earlier_first, segments, positions))
    return outputs

def reference(layer_in, earlier_outs, cotangent, segments, positions, w_qkv, w_out, w_up, w_down, ln_gains, ln_biases, dwa_weights):

    def wrapped(resid_in, earlier, qkv_weight, out_weight, up_weight, down_weight, ln_gain, ln_bias, dwa_mix):
        return forward(resid_in, earlier, qkv_weight, out_weight, up_weight, down_weight, ln_gain, ln_bias, dwa_mix, segments, positions)
    result, pullback = jax.vjp(wrapped, layer_in.astype(jnp.float32), earlier_outs.astype(jnp.float32), w_qkv.astype(jnp.float32), w_out.astype(jnp.float32), w_up.astype(jnp.float32), w_down.astype(jnp.float32), ln_gains.astype(jnp.float32), ln_biases.astype(jnp.float32), dwa_weights.astype(jnp.float32))
    grads = pullback(cotangent.astype(jnp.float32))
    return (result.astype(jnp.bfloat16), grads[0], grads[1], grads[2], grads[3], grads[4], grads[5], grads[6], grads[7], grads[8])
```

```python
import functools
import math

import jax
import jax.numpy as jnp
from jax import lax
from jax.experimental import pallas as pl
from jax.experimental.pallas import tpu as pltpu
from jax.sharding import PartitionSpec as P

HEAD = 64
SEQ_MIN = 1024
SEQ_DEV = 64
EPSILON = 1e-05
NEG_FILL = -1e30
F32 = jnp.float32
B16 = jnp.bfloat16
NT = (((1,), (1,)), ((), ()))
NN = (((1,), (0,)), ((), ()))
TN = (((0,), (0,)), ((), ()))
PARAMS = pltpu.CompilerParams(vmem_limit_bytes=48 << 20)


def normalize(values):
    centre = values - jnp.mean(values, axis=-1, keepdims=True)
    spread = lax.rsqrt(jnp.mean(centre * centre, axis=-1, keepdims=True) + EPSILON)
    return (centre * spread, spread)


def norm_back(grad_normed, scaled, spread, ln_gain):
    shaped = grad_normed * ln_gain
    return spread * (
        shaped
        - jnp.mean(shaped, axis=-1, keepdims=True)
        - scaled * jnp.mean(shaped * scaled, axis=-1, keepdims=True)
    )


def rotary_tables(places, width):
    half_size = HEAD // 2
    inverse = 10000.0 ** (-(jnp.arange(half_size, dtype=F32) * 2.0) / HEAD)
    angles = places.astype(F32)[:, None] * inverse[None, :]
    cos_part, sin_part = lax.optimization_barrier((jnp.cos(angles), jnp.sin(angles)))
    return (
        jnp.tile(cos_part, (1, 2 * width // HEAD)),
        jnp.tile(jnp.concatenate([-sin_part, sin_part], axis=1), (1, width // HEAD)),
    )


def swap_halves(values):
    width = values.shape[-1]
    half = HEAD // 2
    if width % 128 == 0:
        lane = lax.broadcasted_iota(jnp.int32, values.shape, 1)
        return jnp.where(
            lane % HEAD < half,
            pltpu.roll(values, width - half, 1),
            pltpu.roll(values, half, 1),
        )
    return jnp.concatenate([values[:, half:], values[:, :half]], axis=-1)


def side_by_side(parts):
    return jnp.concatenate(parts, axis=-1) if len(parts) > 1 else parts[0]


def piece_at(spot_ref, t, piece):
    return pl.ds(pl.multiple_of(spot_ref[t] * piece, piece), piece)


def doc_mask_of(seg_col, seg_row, lo, hi):
    shape = (hi, hi - lo)
    causal = lax.broadcasted_iota(jnp.int32, shape, 0) <= lo + lax.broadcasted_iota(
        jnp.int32, shape, 1
    )
    return (seg_col[:hi] == seg_row[:, lo:hi]) & causal


def attend_forward(
    spot_ref, q_in, k_in, v_in, cos_ref, sin_ref, seg_col, seg_row, q_ref, k_ref, v_ref, att_ref,
    lse_ref, *, piece, blk
):
    rows, width = q_ref.shape
    score_scale = HEAD ** (-0.5)
    for t in range(rows // piece):
        src = piece_at(spot_ref, t, piece)
        dst = slice(t * piece, (t + 1) * piece)
        cos_part, sin_part = cos_ref[dst], sin_ref[dst]
        q_val, k_val = q_in[src].astype(F32), k_in[src].astype(F32)
        q_ref[dst] = (q_val * cos_part + swap_halves(q_val) * sin_part).astype(B16)
        k_ref[dst] = (k_val * cos_part + swap_halves(k_val) * sin_part).astype(B16)
        v_ref[dst] = v_in[src].astype(B16)
    for t in range(rows // blk):
        lo, hi = t * blk, (t + 1) * blk
        mask = doc_mask_of(seg_col, seg_row, lo, hi)
        outs = []
        for h in range(width // HEAD):
            cols = slice(h * HEAD, (h + 1) * HEAD)
            q_blk = q_ref[lo:hi, cols] * B16(score_scale)
            raw = lax.dot_general(k_ref[:hi, cols], q_blk, NT, preferred_element_type=F32)
            raw = jnp.where(mask, raw, NEG_FILL)
            top = jnp.max(raw, axis=0, keepdims=True)
            terms = jnp.exp(raw - top)
            total = jnp.sum(terms, axis=0, keepdims=True)
            probs = (terms * (1.0 / total)).astype(B16)
            outs.append(
                lax.dot_general(probs, v_ref[:hi, cols], TN, preferred_element_type=F32)
            )
            lse_ref[h, :, lo:hi] = jnp.broadcast_to(top + jnp.log(total), (8, blk))
        att = side_by_side(outs).astype(B16)
        for u in range(blk // piece):
            dst = piece_at(spot_ref, t * (blk // piece) + u, piece)
            att_ref[dst] = att[u * piece : (u + 1) * piece]


def attend_backward(
    spot_ref, q_ref, k_ref, v_ref, g_in, lse_ref, cos_ref, sin_ref, seg_col, seg_row, out_ref,
    g_ref, dk_acc, dv_acc, dq_acc, *, piece, blk
):
    rows, width = q_ref.shape
    score_scale = HEAD ** (-0.5)
    for t in range(rows // piece):
        g_ref[t * piece : (t + 1) * piece] = g_in[piece_at(spot_ref, t, piece)]
    for t in reversed(range(rows // blk)):
        lo, hi = t * blk, (t + 1) * blk
        mask = doc_mask_of(seg_col, seg_row, lo, hi)
        dqs, dks, dvs = [], [], []
        for h in range(width // HEAD):
            cols = slice(h * HEAD, (h + 1) * HEAD)
            q_blk, g_blk = q_ref[lo:hi, cols] * B16(score_scale), g_ref[lo:hi, cols]
            raw = lax.dot_general(k_ref[:hi, cols], q_blk, NT, preferred_element_type=F32)
            probs = jnp.exp(jnp.where(mask, raw, NEG_FILL) - lse_ref[h, :1, lo:hi])
            gp = lax.dot_general(v_ref[:hi, cols], g_blk, NT, preferred_element_type=F32)
            inner = jnp.sum(probs * gp, axis=0, keepdims=True)
            gs = (probs * (gp - inner)).astype(B16)
            dvs.append(
                lax.dot_general(probs.astype(B16), g_blk, NN, preferred_element_type=F32)
            )
            dks.append(lax.dot_general(gs, q_blk, NN, preferred_element_type=F32))
            dqs.append(
                lax.dot_general(gs, k_ref[:hi, cols], TN, preferred_element_type=F32)
                * score_scale
            )
        dq_acc[lo:hi] = side_by_side(dqs)
        if hi == rows:
            dk_acc[...] = side_by_side(dks)
            dv_acc[...] = side_by_side(dvs)
        else:
            dk_acc[:hi] += side_by_side(dks)
            dv_acc[:hi] += side_by_side(dvs)
    for t in range(rows // piece):
        dst = piece_at(spot_ref, t, piece)
        src = slice(t * piece, (t + 1) * piece)
        cos_part, sin_part = cos_ref[src], sin_ref[src]
        dq, dk = dq_acc[src], dk_acc[src]
        out_ref[0, dst] = (dq * cos_part - swap_halves(dq) * sin_part).astype(B16)
        out_ref[1, dst] = (dk * cos_part - swap_halves(dk) * sin_part).astype(B16)
        out_ref[2, dst] = dv_acc[src].astype(B16)


def attention_specs(rows, lanes, seq_len):
    width = min(128, lanes)
    return (
        width,
        (lanes // width, rows // seq_len),
        pl.BlockSpec((seq_len, width), lambda i, j, *_: (j, i)),
        pl.BlockSpec((seq_len, width), lambda i, j, *_: (j, 0)),
        pl.BlockSpec((seq_len, 1), lambda i, j, *_: (j, 0)),
        pl.BlockSpec((1, seq_len), lambda i, j, *_: (0, j)),
        pl.BlockSpec((width // HEAD, 8, seq_len), lambda i, j, *_: (i, 0, j)),
    )


def attention(spots, proj, tables, seg_cols, seg_rows, seq_len, piece):
    _, rows, lanes = proj.shape
    width, grid, wide, table, col, row, stat = attention_specs(rows, lanes, seq_len)
    planes = [
        pl.BlockSpec((None, seq_len, width), lambda i, j, *_, n=n: (n, j, i)) for n in range(3)
    ]
    full = jax.ShapeDtypeStruct((rows, lanes), B16)
    return pl.pallas_call(
        functools.partial(attend_forward, piece=piece, blk=min(256, seq_len)),
        out_shape=(full,) * 4 + (jax.ShapeDtypeStruct((lanes // HEAD, 8, rows), F32),),
        grid_spec=pltpu.PrefetchScalarGridSpec(
            num_scalar_prefetch=1,
            grid=grid,
            in_specs=planes + [table, table, col, row],
            out_specs=(wide, wide, wide, wide, stat),
        ),
        compiler_params=PARAMS,
        cost_estimate=pl.CostEstimate(
            flops=16 * rows * seq_len * lanes,
            bytes_accessed=rows * lanes * 24,
            transcendentals=rows * seq_len * lanes // HEAD,
        ),
        name="attend_forward",
    )(spots, proj, proj, proj, *tables, seg_cols, seg_rows)


def attention_back(spots, saved, grad, tables, seg_cols, seg_rows, seq_len, piece):
    q, k, v, lse = saved
    rows, lanes = q.shape
    width, grid, wide, table, col, row, stat = attention_specs(rows, lanes, seq_len)
    return pl.pallas_call(
        functools.partial(attend_backward, piece=piece, blk=min(256, seq_len)),
        out_shape=jax.ShapeDtypeStruct((3, rows, lanes), B16),
        grid_spec=pltpu.PrefetchScalarGridSpec(
            num_scalar_prefetch=1,
            grid=grid,
            in_specs=[wide, wide, wide, wide, stat, table, table, col, row],
            out_specs=pl.BlockSpec((3, seq_len, width), lambda i, j, *_: (0, j, i)),
            scratch_shapes=[pltpu.VMEM((seq_len, width), B16)]
            + [pltpu.VMEM((seq_len, width), F32)] * 3,
        ),
        compiler_params=PARAMS,
        cost_estimate=pl.CostEstimate(
            flops=24 * rows * seq_len * lanes,
            bytes_accessed=rows * lanes * 24,
            transcendentals=rows * seq_len * lanes // HEAD,
        ),
        name="attend_backward",
    )(spots, q, k, v, grad, lse, *tables, seg_cols, seg_rows)


def expand_kernel(x_ref, w_ref, hidden_ref, slope_ref):
    pre = jnp.dot(x_ref[...], w_ref[...], preferred_element_type=F32)
    share = 0.5 * (1.0 + lax.erf(pre * (2.0**-0.5)))
    hidden_ref[...] = (pre * share).astype(B16)
    density = jnp.exp(-0.5 * pre * pre) * ((2.0 * math.pi) ** -0.5)
    slope_ref[...] = (share + pre * density).astype(B16)


def expand(rows_in, weight):
    rows, depth = rows_in.shape
    units = weight.shape[1]
    tile, strip = min(256, units), min(512, rows)
    out = pl.BlockSpec((strip, tile), lambda i, j: (i, j))
    full = jax.ShapeDtypeStruct((rows, units), B16)
    return pl.pallas_call(
        expand_kernel,
        out_shape=(full, full),
        grid=(rows // strip, units // tile),
        in_specs=[
            pl.BlockSpec((strip, depth), lambda i, j: (i, 0)),
            pl.BlockSpec((depth, tile), lambda i, j: (0, j)),
        ],
        out_specs=(out, out),
        compiler_params=PARAMS,
        cost_estimate=pl.CostEstimate(
            flops=2 * rows * depth * units,
            bytes_accessed=2 * (rows * depth + depth * units) + 4 * rows * units,
            transcendentals=2 * rows * units,
        ),
        name="expand",
    )(rows_in, weight)


def row_chunks(refs, size):
    return [
        ref.at[slice(lo, lo + size)] for ref in refs for lo in range(0, ref.shape[-2], size)
    ]


def weight_kernel(*refs, x_count, planes, size, splits):
    xs, ys, out_ref = refs[:x_count], refs[x_count:-1], refs[-1]
    chunks = row_chunks(xs, size)
    for plane in range(planes or 1):
        own = [ref.at[plane] for ref in ys] if planes else ys
        acc = None
        for x_part, y_part in zip(chunks, row_chunks(own, size)):
            term = lax.dot_general(x_part[...], y_part[...], TN, preferred_element_type=F32)
            acc = term if acc is None else acc + term
        acc = acc.astype(B16)
        if planes:
            out_ref[plane] = acc
        elif splits:
            step = acc.shape[1] // splits
            for n in range(splits):
                out_ref[n] = acc[:, n * step : (n + 1) * step]
        else:
            out_ref[...] = acc


def weight_grad(xs, ys, out_shape, out_block, out_index, x_tile, y_tile, planes=0, splits=0):
    x_rows, depth = sum(x.shape[0] for x in xs), xs[0].shape[1]
    width = ys[0].shape[-1]
    size = math.gcd(512, *[x.shape[0] for x in xs], *[y.shape[-2] for y in ys])
    x_specs = [pl.BlockSpec((x.shape[0], x_tile), lambda i, j: (0, i)) for x in xs]
    y_specs = [
        pl.BlockSpec((planes, y.shape[1], y_tile), lambda i, j: (0, 0, j))
        if planes
        else pl.BlockSpec((y.shape[0], y_tile), lambda i, j: (0, j))
        for y in ys
    ]
    return pl.pallas_call(
        functools.partial(
            weight_kernel, x_count=len(xs), planes=planes, size=size, splits=splits
        ),
        out_shape=jax.ShapeDtypeStruct(out_shape, B16),
        grid=(depth // x_tile, width // y_tile),
        in_specs=x_specs + y_specs,
        out_specs=pl.BlockSpec(out_block, out_index),
        compiler_params=PARAMS,
        cost_estimate=pl.CostEstimate(
            flops=2 * x_rows * depth * width * max(1, planes),
            bytes_accessed=2 * (x_rows * (depth + width) + depth * width),
            transcendentals=0,
        ),
        name="weight_grad",
    )(*xs, *ys)


def flip(values, bits):
    count = lax.axis_size("col")
    return lax.ppermute(values, "col", [(i, i ^ bits) for i in range(count)])


def spread(values, direct):
    if not direct:
        return [lax.all_gather(values, "col", axis=0, tiled=True)]
    chips = lax.axis_size("col") // 2
    near = jnp.concatenate([values] + [flip(values, 2 * c) for c in range(1, chips)], axis=0)
    return [near, flip(near, 1)]


def collapse(make, direct):
    if not direct:
        return lax.psum_scatter(
            make(0).astype(B16), "col", scatter_dimension=0, tiled=True
        ).astype(F32)
    chips = lax.axis_size("col") // 2
    got = flip(make(1).astype(B16), 1)
    near = (make(0) + got.astype(F32)).astype(B16)
    size = near.shape[0] // chips
    total = near[:size].astype(F32)
    for c in range(1, chips):
        total = total + flip(near[c * size : (c + 1) * size], 2 * c).astype(F32)
    return total


def row_shift(values, step):
    count = lax.axis_size("row")
    return lax.ppermute(values, "row", [(i, (i + step) % count) for i in range(count)])


def body(
    layer_in,
    earlier_outs,
    cotangent,
    segments,
    positions,
    w_qkv,
    w_out,
    w_up,
    w_down,
    ln_gains,
    ln_biases,
    dwa_weights,
):
    micro_count, tok_dev, model_width = layer_in.shape
    prior_count = earlier_outs.shape[0]
    col_count = lax.axis_size("col")
    row_count = lax.axis_size("row")
    row_me, col_me = lax.axis_index("row"), lax.axis_index("col")
    direct = col_count == 8
    seq_len = max(SEQ_MIN, SEQ_DEV * col_count)
    group_rows = tok_dev * col_count
    lanes = w_qkv.shape[2]
    part_width = model_width // row_count
    units = w_up.shape[1]
    micros = range(micro_count)

    piece_ids = jnp.arange(col_count, dtype=jnp.int32)
    if direct:
        code = piece_ids ^ col_me
        spots = (code & 1) * (col_count // 2) + (code >> 1)
    else:
        spots = piece_ids

    packed = jnp.concatenate([ln_gains, ln_biases], axis=0)
    norm_params = jnp.zeros((row_count,) + packed.shape, B16)
    norm_params = lax.dynamic_update_index_in_dim(norm_params, packed, row_me, 0)
    for step in range(1, row_count):
        norm_params = lax.dynamic_update_index_in_dim(
            norm_params, row_shift(packed, step), (row_me - step) % row_count, 0
        )
    norm_params = jnp.moveaxis(norm_params, 0, 1).reshape(4, model_width).astype(F32)
    ln_gain, ln_bias = norm_params[:2], norm_params[2:]

    qkv_full = lax.all_gather(w_qkv, "row", axis=1, tiled=True)
    out_full = lax.all_gather(w_out, "row", axis=1, tiled=True)
    up_full = lax.all_gather(w_up, "row", axis=0, tiled=True)
    down_full = lax.all_gather(w_down, "row", axis=1, tiled=True)

    tables = [rotary_tables(positions[m], min(128, lanes)) for m in micros]
    seg_cols = [segments[m][:, None] for m in micros]
    seg_rows = [segments[m][None, :] for m in micros]

    resid_in = [layer_in[m].astype(F32) for m in micros]
    first = [normalize(v) for v in resid_in]
    normed1 = [(s * ln_gain[0] + ln_bias[0]).astype(B16) for s, _ in first]
    rows_one = [spread(v, direct) for v in normed1]
    grad_y = [cotangent[m].astype(F32) for m in micros]
    grad_block = [dwa_weights[prior_count] * g for g in grad_y]
    grad_rows = [spread(g.astype(B16), direct) for g in grad_block]
    parts = range(len(rows_one[0]))
    part_rows = group_rows // len(parts)

    def part_of(values, n):
        return values[n * part_rows : (n + 1) * part_rows]

    saved, attended = [], []
    for m in micros:
        proj = jnp.concatenate(
            [
                jnp.einsum("sd,jdh->jsh", v, qkv_full, preferred_element_type=F32)
                for v in rows_one[m]
            ],
            axis=1,
        )
        q, k, v, att, lse = attention(
            spots, proj, tables[m], seg_cols[m], seg_rows[m], seq_len, tok_dev
        )
        saved.append((q, k, v, lse))
        attended.append(att)

    resid, second, rows_two = [], [], []
    for m in micros:
        mixed = collapse(
            lambda n: jnp.dot(part_of(attended[m], n), out_full, preferred_element_type=F32),
            direct,
        )
        resid.append(resid_in[m] + mixed)
        second.append(normalize(resid[m]))
        normed2 = (second[m][0] * ln_gain[1] + ln_bias[1]).astype(B16)
        rows_two.append(spread(normed2, direct))

    hidden, grad_pre, grad_normed2 = [], [], []
    for m in micros:
        pairs = [expand(v, up_full) for v in rows_two[m]]
        hidden.append([a for a, _ in pairs])
        grad_pre.append(
            [
                (
                    slope.astype(F32)
                    * jnp.einsum("sd,fd->sf", g, down_full, preferred_element_type=F32)
                ).astype(B16)
                for (_, slope), g in zip(pairs, grad_rows[m])
            ]
        )
        grad_normed2.append(
            collapse(
                lambda n: jnp.einsum(
                    "sf,df->sd", grad_pre[m][n], up_full, preferred_element_type=F32
                ),
                direct,
            )
        )

    flat = lambda lists: [v for parts_of in lists for v in parts_of]
    total_rows = micro_count * group_rows
    fit = max(128, (8 << 20) // (2 * total_rows))
    x_tile, y_tile = min(256, units), min(model_width, fit)
    splits = y_tile // part_width if y_tile > part_width else 0
    y_blocks = part_width // y_tile if y_tile < part_width else 1
    grad_down = weight_grad(
        flat(hidden),
        flat(grad_rows),
        (row_count, units, part_width),
        (splits, x_tile, part_width) if splits else (None, x_tile, y_tile),
        (lambda i, j: (j, i, 0)) if splits else (lambda i, j: (j // y_blocks, i, j % y_blocks)),
        x_tile,
        y_tile,
        splits=splits,
    )
    grad_down = lax.psum_scatter(grad_down, "row", scatter_dimension=0)
    x_tile, y_tile = min(256, model_width), min(units, fit)
    grad_up = weight_grad(
        flat(rows_two),
        flat(grad_pre),
        (model_width, units),
        (x_tile, y_tile),
        lambda i, j: (i, j),
        x_tile,
        y_tile,
    )
    grad_up = lax.psum_scatter(grad_up, "row", scatter_dimension=0, tiled=True)

    outputs, mix_grads = [], []
    for m in micros:
        branch = collapse(
            lambda n: jnp.dot(hidden[m][n], down_full, preferred_element_type=F32), direct
        )
        block_out = resid[m] + branch
        earlier = earlier_outs[:, m].astype(F32)
        mix_sum = dwa_weights[0] * earlier[0]
        for level in range(1, prior_count):
            mix_sum = mix_sum + dwa_weights[level] * earlier[level]
        outputs.append((mix_sum + dwa_weights[prior_count] * block_out).astype(B16))
        mix_grads.append(
            jnp.concatenate(
                [
                    jnp.sum(grad_y[m][None] * earlier, axis=(1, 2)),
                    jnp.sum(grad_y[m] * block_out)[None],
                ]
            )
        )

    grad_resid, grad_mixed_rows, grad_planes = [], [], []
    for m in micros:
        grad_resid.append(grad_block[m] + norm_back(grad_normed2[m], *second[m], ln_gain[1]))
        grad_mixed_rows.append(spread(grad_resid[m].astype(B16), direct))
        grad_att = jnp.concatenate(
            [
                jnp.einsum("sd,hd->sh", v, out_full, preferred_element_type=F32).astype(B16)
                for v in grad_mixed_rows[m]
            ],
            axis=0,
        )
        grad_planes.append(
            attention_back(
                spots, saved[m], grad_att, tables[m], seg_cols[m], seg_rows[m], seq_len, tok_dev
            )
        )

    grad_wout = weight_grad(
        attended,
        flat(grad_mixed_rows),
        (row_count, lanes, part_width),
        (None, lanes, part_width),
        lambda i, j: (j, i, 0),
        lanes,
        part_width,
    )
    grad_wout = lax.psum_scatter(grad_wout, "row", scatter_dimension=0)
    x_tile = min(256, part_width)
    per_block = part_width // x_tile
    grad_qkv = weight_grad(
        flat(rows_one),
        grad_planes,
        (row_count, 3, part_width, lanes),
        (None, 3, x_tile, lanes),
        lambda i, j: (i // per_block, 0, i % per_block, 0),
        x_tile,
        lanes,
        planes=3,
    )
    grad_qkv = lax.psum_scatter(grad_qkv, "row", scatter_dimension=0)

    in_grads, grad_normed1 = [], []
    for m in micros:
        grad_normed1.append(
            collapse(
                lambda n: jnp.einsum(
                    "jsh,jdh->sd",
                    grad_planes[m][:, n * part_rows : (n + 1) * part_rows],
                    qkv_full,
                    preferred_element_type=F32,
                ),
                direct,
            )
        )
        in_grads.append(grad_resid[m] + norm_back(grad_normed1[m], *first[m], ln_gain[0]))

    stats = jnp.stack(
        [
            sum(jnp.sum(grad_normed1[m] * first[m][0], axis=0) for m in micros),
            sum(jnp.sum(grad_normed2[m] * second[m][0], axis=0) for m in micros),
            sum(jnp.sum(grad_normed1[m], axis=0) for m in micros),
            sum(jnp.sum(grad_normed2[m], axis=0) for m in micros),
        ]
    )
    mix_row = jnp.pad(sum(mix_grads), (0, part_width - prior_count - 1))
    slabs = jnp.concatenate(
        [
            jnp.moveaxis(stats.reshape(4, row_count, part_width), 1, 0),
            jnp.broadcast_to(mix_row, (row_count, 4, part_width)),
        ],
        axis=1,
    )
    slab = lax.dynamic_index_in_dim(slabs, row_me, 0, keepdims=False)
    for step in range(1, row_count):
        leaving = lax.dynamic_index_in_dim(slabs, (row_me + step) % row_count, 0, keepdims=False)
        slab = slab + row_shift(leaving, step)
    bits = 1
    while bits < col_count:
        slab = slab + flip(slab, bits)
        bits *= 2

    grad_earlier = (
        dwa_weights[:prior_count, None, None, None] * cotangent.astype(F32)[None]
    )
    return (
        jnp.stack(outputs),
        jnp.stack(in_grads),
        grad_earlier,
        grad_qkv.astype(F32),
        grad_wout.astype(F32),
        grad_up.astype(F32),
        grad_down.astype(F32),
        slab[:2],
        slab[2:4],
        slab[4, : prior_count + 1],
    )


def solution(mesh):
    in_specs = (
        P(None, ("row", "col"), None),
        P(None, None, ("row", "col"), None),
        P(None, ("row", "col"), None),
        P(None, "row"),
        P(None, "row"),
        P(None, "row", "col"),
        P("col", "row"),
        P("row", "col"),
        P("col", "row"),
        P(None, "row"),
        P(None, "row"),
        P(),
    )
    out_specs = (
        P(None, ("row", "col"), None),
        P(None, ("row", "col"), None),
        P(None, None, ("row", "col"), None),
        P(None, "row", "col"),
        P("col", "row"),
        P("row", "col"),
        P("col", "row"),
        P(None, "row"),
        P(None, "row"),
        P(),
    )
    return jax.shard_map(body, mesh=mesh, in_specs=in_specs, out_specs=out_specs, check_vma=False)
```

```python
import functools
import math

import jax
import jax.numpy as jnp
from jax import lax
from jax.experimental import pallas as pl
from jax.experimental.pallas import tpu as pltpu
from jax.sharding import PartitionSpec as P

HEAD = 64
SEQ_MIN = 1024
SEQ_DEV = 64
EPSILON = 1e-05
NEG_FILL = -1e30
F32 = jnp.float32
B16 = jnp.bfloat16
NT = (((1,), (1,)), ((), ()))
NN = (((1,), (0,)), ((), ()))
TN = (((0,), (0,)), ((), ()))
PARAMS = pltpu.CompilerParams(vmem_limit_bytes=48 << 20)


def normalize(values):
    centre = values - jnp.mean(values, axis=-1, keepdims=True)
    spread = lax.rsqrt(jnp.mean(centre * centre, axis=-1, keepdims=True) + EPSILON)
    return (centre * spread, spread)


def norm_back(grad_normed, scaled, spread, ln_gain):
    shaped = grad_normed * ln_gain
    return spread * (
        shaped
        - jnp.mean(shaped, axis=-1, keepdims=True)
        - scaled * jnp.mean(shaped * scaled, axis=-1, keepdims=True)
    )


def rotary_tables(places, width):
    half_size = HEAD // 2
    inverse = 10000.0 ** (-(jnp.arange(half_size, dtype=F32) * 2.0) / HEAD)
    angles = places.astype(F32)[:, None] * inverse[None, :]
    cos_part, sin_part = lax.optimization_barrier((jnp.cos(angles), jnp.sin(angles)))
    return (
        jnp.tile(cos_part, (1, 2 * width // HEAD)),
        jnp.tile(jnp.concatenate([-sin_part, sin_part], axis=1), (1, width // HEAD)),
    )


def swap_halves(values):
    width = values.shape[-1]
    half = HEAD // 2
    if width % 128 == 0:
        lane = lax.broadcasted_iota(jnp.int32, values.shape, 1)
        return jnp.where(
            lane % HEAD < half,
            pltpu.roll(values, width - half, 1),
            pltpu.roll(values, half, 1),
        )
    return jnp.concatenate([values[:, half:], values[:, :half]], axis=-1)


def side_by_side(parts):
    return jnp.concatenate(parts, axis=-1) if len(parts) > 1 else parts[0]


def piece_at(spot_ref, t, piece):
    return pl.ds(pl.multiple_of(spot_ref[t] * piece, piece), piece)


def doc_mask_of(seg_col, seg_row, lo, hi):
    shape = (hi, hi - lo)
    causal = lax.broadcasted_iota(jnp.int32, shape, 0) <= lo + lax.broadcasted_iota(
        jnp.int32, shape, 1
    )
    return (seg_col[:hi] == seg_row[:, lo:hi]) & causal


def attend_forward(
    spot_ref, q_in, k_in, v_in, cos_ref, sin_ref, seg_col, seg_row, q_ref, k_ref, v_ref, att_ref,
    lse_ref, *, piece, blk
):
    rows, width = q_ref.shape
    score_scale = HEAD ** (-0.5)
    for t in range(rows // piece):
        src = piece_at(spot_ref, t, piece)
        dst = slice(t * piece, (t + 1) * piece)
        cos_part, sin_part = cos_ref[dst], sin_ref[dst]
        q_val, k_val = q_in[src].astype(F32), k_in[src].astype(F32)
        q_ref[dst] = (q_val * cos_part + swap_halves(q_val) * sin_part).astype(B16)
        k_ref[dst] = (k_val * cos_part + swap_halves(k_val) * sin_part).astype(B16)
        v_ref[dst] = v_in[src].astype(B16)
    for t in range(rows // blk):
        lo, hi = t * blk, (t + 1) * blk
        mask = doc_mask_of(seg_col, seg_row, lo, hi)
        outs = []
        for h in range(width // HEAD):
            cols = slice(h * HEAD, (h + 1) * HEAD)
            q_blk = q_ref[lo:hi, cols] * B16(score_scale)
            raw = lax.dot_general(k_ref[:hi, cols], q_blk, NT, preferred_element_type=F32)
            raw = jnp.where(mask, raw, NEG_FILL)
            top = jnp.max(raw, axis=0, keepdims=True)
            terms = jnp.exp(raw - top)
            total = jnp.sum(terms, axis=0, keepdims=True)
            probs = (terms * (1.0 / total)).astype(B16)
            outs.append(
                lax.dot_general(probs, v_ref[:hi, cols], TN, preferred_element_type=F32)
            )
            lse_ref[h, :, lo:hi] = jnp.broadcast_to(top + jnp.log(total), (8, blk))
        att = side_by_side(outs).astype(B16)
        for u in range(blk // piece):
            dst = piece_at(spot_ref, t * (blk // piece) + u, piece)
            att_ref[dst] = att[u * piece : (u + 1) * piece]


def attend_backward(
    spot_ref, q_ref, k_ref, v_ref, g_in, lse_ref, cos_ref, sin_ref, seg_col, seg_row, out_ref,
    g_ref, dk_acc, dv_acc, dq_acc, *, piece, blk
):
    rows, width = q_ref.shape
    score_scale = HEAD ** (-0.5)
    for t in range(rows // piece):
        g_ref[t * piece : (t + 1) * piece] = g_in[piece_at(spot_ref, t, piece)]
    for t in reversed(range(rows // blk)):
        lo, hi = t * blk, (t + 1) * blk
        mask = doc_mask_of(seg_col, seg_row, lo, hi)
        dqs, dks, dvs = [], [], []
        for h in range(width // HEAD):
            cols = slice(h * HEAD, (h + 1) * HEAD)
            q_blk, g_blk = q_ref[lo:hi, cols] * B16(score_scale), g_ref[lo:hi, cols]
            raw = lax.dot_general(k_ref[:hi, cols], q_blk, NT, preferred_element_type=F32)
            probs = jnp.exp(jnp.where(mask, raw, NEG_FILL) - lse_ref[h, :1, lo:hi])
            gp = lax.dot_general(v_ref[:hi, cols], g_blk, NT, preferred_element_type=F32)
            inner = jnp.sum(probs * gp, axis=0, keepdims=True)
            gs = (probs * (gp - inner)).astype(B16)
            dvs.append(
                lax.dot_general(probs.astype(B16), g_blk, NN, preferred_element_type=F32)
            )
            dks.append(lax.dot_general(gs, q_blk, NN, preferred_element_type=F32))
            dqs.append(
                lax.dot_general(gs, k_ref[:hi, cols], TN, preferred_element_type=F32)
                * score_scale
            )
        dq_acc[lo:hi] = side_by_side(dqs)
        if hi == rows:
            dk_acc[...] = side_by_side(dks)
            dv_acc[...] = side_by_side(dvs)
        else:
            dk_acc[:hi] += side_by_side(dks)
            dv_acc[:hi] += side_by_side(dvs)
    for t in range(rows // piece):
        dst = piece_at(spot_ref, t, piece)
        src = slice(t * piece, (t + 1) * piece)
        cos_part, sin_part = cos_ref[src], sin_ref[src]
        dq, dk = dq_acc[src], dk_acc[src]
        out_ref[0, dst] = (dq * cos_part - swap_halves(dq) * sin_part).astype(B16)
        out_ref[1, dst] = (dk * cos_part - swap_halves(dk) * sin_part).astype(B16)
        out_ref[2, dst] = dv_acc[src].astype(B16)


def attention_specs(rows, lanes, seq_len):
    width = min(128, lanes)
    return (
        width,
        (lanes // width, rows // seq_len),
        pl.BlockSpec((seq_len, width), lambda i, j, *_: (j, i)),
        pl.BlockSpec((seq_len, width), lambda i, j, *_: (j, 0)),
        pl.BlockSpec((seq_len, 1), lambda i, j, *_: (j, 0)),
        pl.BlockSpec((1, seq_len), lambda i, j, *_: (0, j)),
        pl.BlockSpec((width // HEAD, 8, seq_len), lambda i, j, *_: (i, 0, j)),
    )


def attention(spots, proj, tables, seg_cols, seg_rows, seq_len, piece):
    _, rows, lanes = proj.shape
    width, grid, wide, table, col, row, stat = attention_specs(rows, lanes, seq_len)
    planes = [
        pl.BlockSpec((None, seq_len, width), lambda i, j, *_, n=n: (n, j, i)) for n in range(3)
    ]
    full = jax.ShapeDtypeStruct((rows, lanes), B16)
    return pl.pallas_call(
        functools.partial(attend_forward, piece=piece, blk=min(256, seq_len)),
        out_shape=(full,) * 4 + (jax.ShapeDtypeStruct((lanes // HEAD, 8, rows), F32),),
        grid_spec=pltpu.PrefetchScalarGridSpec(
            num_scalar_prefetch=1,
            grid=grid,
            in_specs=planes + [table, table, col, row],
            out_specs=(wide, wide, wide, wide, stat),
        ),
        compiler_params=PARAMS,
        cost_estimate=pl.CostEstimate(
            flops=16 * rows * seq_len * lanes,
            bytes_accessed=rows * lanes * 24,
            transcendentals=rows * seq_len * lanes // HEAD,
        ),
        name="attend_forward",
    )(spots, proj, proj, proj, *tables, seg_cols, seg_rows)


def attention_back(spots, saved, grad, tables, seg_cols, seg_rows, seq_len, piece):
    q, k, v, lse = saved
    rows, lanes = q.shape
    width, grid, wide, table, col, row, stat = attention_specs(rows, lanes, seq_len)
    return pl.pallas_call(
        functools.partial(attend_backward, piece=piece, blk=min(256, seq_len)),
        out_shape=jax.ShapeDtypeStruct((3, rows, lanes), B16),
        grid_spec=pltpu.PrefetchScalarGridSpec(
            num_scalar_prefetch=1,
            grid=grid,
            in_specs=[wide, wide, wide, wide, stat, table, table, col, row],
            out_specs=pl.BlockSpec((3, seq_len, width), lambda i, j, *_: (0, j, i)),
            scratch_shapes=[pltpu.VMEM((seq_len, width), B16)]
            + [pltpu.VMEM((seq_len, width), F32)] * 3,
        ),
        compiler_params=PARAMS,
        cost_estimate=pl.CostEstimate(
            flops=24 * rows * seq_len * lanes,
            bytes_accessed=rows * lanes * 24,
            transcendentals=rows * seq_len * lanes // HEAD,
        ),
        name="attend_backward",
    )(spots, q, k, v, grad, lse, *tables, seg_cols, seg_rows)


def expand_kernel(x_ref, w_ref, hidden_ref, slope_ref):
    pre = jnp.dot(x_ref[...], w_ref[...], preferred_element_type=F32)
    share = 0.5 * (1.0 + lax.erf(pre * (2.0**-0.5)))
    hidden_ref[...] = (pre * share).astype(B16)
    density = jnp.exp(-0.5 * pre * pre) * ((2.0 * math.pi) ** -0.5)
    slope_ref[...] = (share + pre * density).astype(B16)


def expand(rows_in, weight):
    rows, depth = rows_in.shape
    units = weight.shape[1]
    tile, strip = min(256, units), min(512, rows)
    out = pl.BlockSpec((strip, tile), lambda i, j: (i, j))
    full = jax.ShapeDtypeStruct((rows, units), B16)
    return pl.pallas_call(
        expand_kernel,
        out_shape=(full, full),
        grid=(rows // strip, units // tile),
        in_specs=[
            pl.BlockSpec((strip, depth), lambda i, j: (i, 0)),
            pl.BlockSpec((depth, tile), lambda i, j: (0, j)),
        ],
        out_specs=(out, out),
        compiler_params=PARAMS,
        cost_estimate=pl.CostEstimate(
            flops=2 * rows * depth * units,
            bytes_accessed=2 * (rows * depth + depth * units) + 4 * rows * units,
            transcendentals=2 * rows * units,
        ),
        name="expand",
    )(rows_in, weight)


def row_chunks(refs, size):
    return [
        ref.at[slice(lo, lo + size)] for ref in refs for lo in range(0, ref.shape[-2], size)
    ]


def weight_kernel(*refs, x_count, y_count, planes, size, splits, stacked):
    xs, ys, out_ref = refs[:x_count], refs[x_count : x_count + y_count], refs[-1]
    chunks = row_chunks(xs, size)
    for plane in range(planes or 1):
        own = [ref.at[plane] for ref in ys] if planes else ys
        acc = None
        for x_part, y_part in zip(chunks, row_chunks(own, size)):
            term = lax.dot_general(x_part[...], y_part[...], TN, preferred_element_type=F32)
            acc = term if acc is None else acc + term
        acc = acc.astype(B16)
        if planes:
            out_ref[plane] = acc
        elif stacked:
            step = acc.shape[0]
            for n in range(acc.shape[1] // step):
                out_ref[n * step : (n + 1) * step] = acc[:, n * step : (n + 1) * step]
        elif splits:
            step = acc.shape[1] // splits
            for n in range(splits):
                out_ref[n] = acc[:, n * step : (n + 1) * step]
        else:
            out_ref[...] = acc


def weight_grad(
    xs, ys, out_shape, out_block, out_index, x_tile, y_tile, planes=0, splits=0, stacked=False,
    base=None
):
    x_rows, depth = sum(x.shape[0] for x in xs), xs[0].shape[1]
    width = ys[0].shape[-1]
    size = math.gcd(512, *[x.shape[0] for x in xs], *[y.shape[-2] for y in ys])
    x_specs = [pl.BlockSpec((x.shape[0], x_tile), lambda i, j: (0, i)) for x in xs]
    y_specs = [
        pl.BlockSpec((planes, y.shape[1], y_tile), lambda i, j: (0, 0, j))
        if planes
        else pl.BlockSpec((y.shape[0], y_tile), lambda i, j: (0, j))
        for y in ys
    ]
    bases = [] if base is None else [base]
    return pl.pallas_call(
        functools.partial(
            weight_kernel,
            x_count=len(xs),
            y_count=len(ys),
            planes=planes,
            size=size,
            splits=splits,
            stacked=stacked,
        ),
        out_shape=jax.ShapeDtypeStruct(out_shape, B16),
        grid=(depth // x_tile, width // y_tile),
        in_specs=x_specs + y_specs + [pl.BlockSpec(memory_space=pl.ANY) for _ in bases],
        out_specs=pl.BlockSpec(out_block, out_index),
        input_output_aliases={len(xs) + len(ys): 0} if bases else {},
        compiler_params=PARAMS,
        cost_estimate=pl.CostEstimate(
            flops=2 * x_rows * depth * width * max(1, planes),
            bytes_accessed=2 * (x_rows * (depth + width) + depth * width),
            transcendentals=0,
        ),
        name="weight_grad",
    )(*xs, *ys, *bases)


def flip(values, bits):
    count = lax.axis_size("col")
    return lax.ppermute(values, "col", [(i, i ^ bits) for i in range(count)])


def spread(values, direct):
    if not direct:
        return [lax.all_gather(values, "col", axis=0, tiled=True)]
    chips = lax.axis_size("col") // 2
    near = jnp.concatenate([values] + [flip(values, 2 * c) for c in range(1, chips)], axis=0)
    return [near, flip(near, 1)]


def near_sum(make, direct):
    if not direct:
        return make(0).astype(B16)
    got = flip(make(1).astype(B16), 1)
    return (make(0) + got.astype(F32)).astype(B16)


def send_sum(near, direct):
    if not direct:
        return [lax.psum_scatter(near, "col", scatter_dimension=0, tiled=True)]
    chips = lax.axis_size("col") // 2
    size = near.shape[0] // chips
    return [near[:size]] + [
        flip(near[c * size : (c + 1) * size], 2 * c) for c in range(1, chips)
    ]


def add_up(parts):
    return sum(v.astype(F32) for v in parts)


def after(values, *others):
    return lax.optimization_barrier((values, others))[0]


def row_shift(values, step):
    count = lax.axis_size("row")
    return lax.ppermute(values, "row", [(i, (i + step) % count) for i in range(count)])


def body(
    layer_in,
    earlier_outs,
    cotangent,
    segments,
    positions,
    w_qkv,
    w_out,
    w_up,
    w_down,
    ln_gains,
    ln_biases,
    dwa_weights,
):
    micro_count, tok_dev, model_width = layer_in.shape
    prior_count = earlier_outs.shape[0]
    col_count = lax.axis_size("col")
    row_count = lax.axis_size("row")
    row_me, col_me = lax.axis_index("row"), lax.axis_index("col")
    direct = col_count == 8
    seq_len = max(SEQ_MIN, SEQ_DEV * col_count)
    group_rows = tok_dev * col_count
    lanes = w_qkv.shape[2]
    part_width = model_width // row_count
    units = w_up.shape[1]
    micros = range(micro_count)

    piece_ids = jnp.arange(col_count, dtype=jnp.int32)
    if direct:
        code = piece_ids ^ col_me
        spots = (code & 1) * (col_count // 2) + (code >> 1)
    else:
        spots = piece_ids

    packed = jnp.concatenate([ln_gains, ln_biases], axis=0)
    norm_params = jnp.zeros((row_count,) + packed.shape, B16)
    norm_params = lax.dynamic_update_index_in_dim(norm_params, packed, row_me, 0)
    for step in range(1, row_count):
        norm_params = lax.dynamic_update_index_in_dim(
            norm_params, row_shift(packed, step), (row_me - step) % row_count, 0
        )
    norm_params = jnp.moveaxis(norm_params, 0, 1).reshape(4, model_width).astype(F32)
    ln_gain, ln_bias = norm_params[:2], norm_params[2:]

    pieces = part_width // lanes
    w_out = jnp.moveaxis(w_out.reshape(lanes, pieces, lanes), 1, 0).reshape(part_width, lanes)
    four_full = lax.all_gather(
        jnp.concatenate([w_qkv, w_out[None]], axis=0), "row", axis=1, tiled=True
    )
    qkv_full = four_full[:3]
    out_full = jnp.moveaxis(four_full[3].reshape(-1, lanes, lanes), 0, 1).reshape(
        lanes, model_width
    )
    up_full = lax.all_gather(w_up, "row", axis=0, tiled=True)
    down_full = lax.all_gather(w_down, "row", axis=1, tiled=True)

    tables = [rotary_tables(positions[m], min(128, lanes)) for m in micros]
    seg_cols = [segments[m][:, None] for m in micros]
    seg_rows = [segments[m][None, :] for m in micros]

    resid_in = [layer_in[m].astype(F32) for m in micros]
    first = [normalize(v) for v in resid_in]
    normed1 = [(s * ln_gain[0] + ln_bias[0]).astype(B16) for s, _ in first]
    grad_y = [cotangent[m].astype(F32) for m in micros]
    grad_block = [dwa_weights[prior_count] * g for g in grad_y]
    rows_one, grad_rows, last = [], [], None
    for values, found in ((normed1, rows_one), (grad_block, grad_rows)):
        for v in values:
            v = v.astype(B16)
            found.append(spread(v if last is None or found is rows_one else after(v, last), direct))
            last = found[-1][0]
    parts = range(len(rows_one[0]))
    part_rows = group_rows // len(parts)

    def part_of(values, n):
        return values[n * part_rows : (n + 1) * part_rows]

    saved, attended, mixed, mixed_parts = [], [], [], []
    for m in micros:
        rows_m = after(rows_one[m], grad_rows[0][0], mixed[-1:])
        proj = jnp.concatenate(
            [
                jnp.einsum("sd,jdh->jsh", v, qkv_full, preferred_element_type=F32)
                for v in rows_m
            ],
            axis=1,
        )
        q, k, v, att, lse = attention(
            spots, proj, tables[m], seg_cols[m], seg_rows[m], seq_len, tok_dev
        )
        saved.append((q, k, v, lse))
        attended.append(att)
        att_m = after(att, mixed_parts[-1] if mixed_parts else grad_rows[-1][0])
        mixed.append(
            near_sum(
                lambda n: jnp.dot(part_of(att_m, n), out_full, preferred_element_type=F32), direct
            )
        )
        mixed_parts.append(send_sum(mixed[-1], direct))

    resid, second, rows_two = [], [], []
    last = []
    for m in micros:
        resid.append(resid_in[m] + add_up(after(mixed_parts[m], last)))
        second.append(normalize(resid[m]))
        normed2 = (second[m][0] * ln_gain[1] + ln_bias[1]).astype(B16)
        rows_two.append(spread(normed2, direct))
        last = normed2

    flat = lambda lists: [v for parts_of in lists for v in parts_of]
    total_rows = micro_count * group_rows
    fit = max(128, (8 << 20) // (2 * total_rows))
    hidden, slopes = [], []
    for m in micros:
        pairs = [expand(v, up_full) for v in rows_two[m]]
        hidden.append([a for a, _ in pairs])
        slopes.append([a for _, a in pairs])
    x_tile, y_tile = min(256, units), min(model_width, fit)
    splits = y_tile // part_width if y_tile > part_width else 0
    y_blocks = part_width // y_tile if y_tile < part_width else 1
    grad_down = weight_grad(
        flat(hidden),
        flat(grad_rows),
        (row_count, units, part_width),
        (splits, x_tile, part_width) if splits else (None, x_tile, y_tile),
        (lambda i, j: (j, i, 0)) if splits else (lambda i, j: (j // y_blocks, i, j % y_blocks)),
        x_tile,
        y_tile,
        splits=splits,
    )
    down_full = after(down_full, grad_down)
    grad_down = lax.psum_scatter(grad_down, "row", scatter_dimension=0)

    grad_pre, back_two = [], []
    for m in micros:
        rows_m = after(grad_rows[m], back_two[-1]) if back_two else grad_rows[m]
        grad_pre.append(
            [
                (
                    slope.astype(F32)
                    * jnp.einsum("sd,fd->sf", g, down_full, preferred_element_type=F32)
                ).astype(B16)
                for slope, g in zip(slopes[m], rows_m)
            ]
        )
        back_two.append(
            near_sum(
                lambda n: jnp.einsum(
                    "sf,df->sd", grad_pre[m][n], up_full, preferred_element_type=F32
                ),
                direct,
            )
        )

    back_parts = [send_sum(v, direct) for v in back_two]
    grad_normed2, grad_resid, grad_mixed_rows = [], [], []
    last = back_two[-1]
    x_tile, y_tile = min(256, model_width), min(units, fit)
    for m in micros:
        grad_normed2.append(add_up(after(back_parts[m], last)))
        grad_resid.append(grad_block[m] + norm_back(grad_normed2[m], *second[m], ln_gain[1]))
        grad_mixed = grad_resid[m].astype(B16)
        grad_mixed_rows.append(spread(grad_mixed, direct))
        if m == 0:
            grad_up = weight_grad(
                flat(rows_two),
                after(flat(grad_pre), grad_mixed),
                (model_width, units),
                (x_tile, y_tile),
                lambda i, j: (i, j),
                x_tile,
                y_tile,
            )
            last = grad_up
    grad_up = lax.psum_scatter(grad_up, "row", scatter_dimension=0, tiled=True)

    branch = []
    for m in micros:
        hidden_m = after(hidden[m], branch[-1] if branch else grad_mixed)
        branch.append(
            near_sum(
                lambda n: jnp.dot(hidden_m[n], down_full, preferred_element_type=F32), direct
            )
        )

    grad_planes = []
    last = branch[-1]
    for m in micros:
        rows_m = after(grad_mixed_rows[m], last)
        grad_att = jnp.concatenate(
            [
                jnp.einsum("sd,hd->sh", v, out_full, preferred_element_type=F32).astype(B16)
                for v in rows_m
            ],
            axis=0,
        )
        grad_planes.append(
            attention_back(
                spots, saved[m], grad_att, tables[m], seg_cols[m], seg_rows[m], seq_len, tok_dev
            )
        )
        last = grad_planes[-1]

    four_shape = (row_count, 4, part_width, lanes)
    grad_four = weight_grad(
        attended,
        flat(grad_mixed_rows),
        four_shape,
        (None, None, part_width, lanes),
        lambda i, j: (j, 3, 0, 0),
        lanes,
        part_width,
        stacked=True,
    )
    x_tile = min(256, part_width)
    per_block = part_width // x_tile
    grad_four = weight_grad(
        flat(rows_one),
        grad_planes,
        four_shape,
        (None, 3, x_tile, lanes),
        lambda i, j: (i // per_block, 0, i % per_block, 0),
        x_tile,
        lanes,
        planes=3,
        base=grad_four,
    )
    last = grad_four
    grad_four = lax.psum_scatter(grad_four, "row", scatter_dimension=0)

    in_grads, grad_normed1, back_one = [], [], []
    for m in micros:
        planes_m = after(grad_planes[m], last)
        back_one.append(
            near_sum(
                lambda n: jnp.einsum(
                    "jsh,jdh->sd",
                    planes_m[:, n * part_rows : (n + 1) * part_rows],
                    qkv_full,
                    preferred_element_type=F32,
                ),
                direct,
            )
        )
        last = back_one[-1]
    for m in micros:
        grad_normed1.append(add_up(send_sum(back_one[m], direct)))
        in_grads.append(grad_resid[m] + norm_back(grad_normed1[m], *first[m], ln_gain[0]))

    outputs, mix_grads = [], []
    for m in micros:
        block_out = resid[m] + add_up(send_sum(branch[m], direct))
        earlier = earlier_outs[:, m].astype(F32)
        mix_sum = dwa_weights[0] * earlier[0]
        for level in range(1, prior_count):
            mix_sum = mix_sum + dwa_weights[level] * earlier[level]
        outputs.append((mix_sum + dwa_weights[prior_count] * block_out).astype(B16))
        mix_grads.append(
            jnp.concatenate(
                [
                    jnp.sum(grad_y[m][None] * earlier, axis=(1, 2)),
                    jnp.sum(grad_y[m] * block_out)[None],
                ]
            )
        )

    stats = jnp.stack(
        [
            sum(jnp.sum(grad_normed1[m] * first[m][0], axis=0) for m in micros),
            sum(jnp.sum(grad_normed2[m] * second[m][0], axis=0) for m in micros),
            sum(jnp.sum(grad_normed1[m], axis=0) for m in micros),
            sum(jnp.sum(grad_normed2[m], axis=0) for m in micros),
        ]
    )
    mix_row = jnp.pad(sum(mix_grads), (0, part_width - prior_count - 1))
    slabs = jnp.concatenate(
        [
            jnp.moveaxis(stats.reshape(4, row_count, part_width), 1, 0),
            jnp.broadcast_to(mix_row, (row_count, 4, part_width)),
        ],
        axis=1,
    )
    slab = lax.dynamic_index_in_dim(slabs, row_me, 0, keepdims=False)
    for step in range(1, row_count):
        leaving = lax.dynamic_index_in_dim(slabs, (row_me + step) % row_count, 0, keepdims=False)
        slab = slab + row_shift(leaving, step)
    bits = 1
    while bits < col_count:
        slab = slab + flip(slab, bits)
        bits *= 2

    grad_earlier = (
        dwa_weights[:prior_count, None, None, None] * cotangent.astype(F32)[None]
    )
    return (
        jnp.stack(outputs),
        jnp.stack(in_grads),
        grad_earlier,
        grad_four[:3].astype(F32),
        jnp.moveaxis(grad_four[3].reshape(pieces, lanes, lanes), 0, 1)
        .reshape(lanes, part_width)
        .astype(F32),
        grad_up.astype(F32),
        grad_down.astype(F32),
        slab[:2],
        slab[2:4],
        slab[4, : prior_count + 1],
    )


def solution(mesh):
    in_specs = (
        P(None, ("row", "col"), None),
        P(None, None, ("row", "col"), None),
        P(None, ("row", "col"), None),
        P(None, "row"),
        P(None, "row"),
        P(None, "row", "col"),
        P("col", "row"),
        P("row", "col"),
        P("col", "row"),
        P(None, "row"),
        P(None, "row"),
        P(),
    )
    out_specs = (
        P(None, ("row", "col"), None),
        P(None, ("row", "col"), None),
        P(None, None, ("row", "col"), None),
        P(None, "row", "col"),
        P("col", "row"),
        P("row", "col"),
        P("col", "row"),
        P(None, "row"),
        P(None, "row"),
        P(),
    )
    return jax.shard_map(body, mesh=mesh, in_specs=in_specs, out_specs=out_specs, check_vma=False)
```

```python
import functools
import math

import jax
import jax.numpy as jnp
from jax import lax
from jax.experimental import pallas as pl
from jax.experimental.pallas import tpu as pltpu
from jax.sharding import PartitionSpec as P

HEAD = 64
SEQ_MIN = 1024
SEQ_DEV = 64
EPSILON = 1e-05
NEG_FILL = -1e30
F32 = jnp.float32
B16 = jnp.bfloat16
NT = (((1,), (1,)), ((), ()))
NN = (((1,), (0,)), ((), ()))
TN = (((0,), (0,)), ((), ()))
PARAMS = pltpu.CompilerParams(vmem_limit_bytes=48 << 20)
SMALL = pltpu.CompilerParams(vmem_limit_bytes=24 << 20)
TINY = pl.CostEstimate(flops=1000, bytes_accessed=1000, transcendentals=0)


def normalize(values):
    centre = values - jnp.mean(values, axis=-1, keepdims=True)
    spread = lax.rsqrt(jnp.mean(centre * centre, axis=-1, keepdims=True) + EPSILON)
    return (centre * spread, spread)


def norm_back(grad_normed, scaled, spread, ln_gain):
    shaped = grad_normed * ln_gain
    return spread * (
        shaped
        - jnp.mean(shaped, axis=-1, keepdims=True)
        - scaled * jnp.mean(shaped * scaled, axis=-1, keepdims=True)
    )


def rotary_tables(places, width):
    half_size = HEAD // 2
    inverse = 10000.0 ** (-(jnp.arange(half_size, dtype=F32) * 2.0) / HEAD)
    angles = places.astype(F32)[:, None] * inverse[None, :]
    cos_part, sin_part = lax.optimization_barrier((jnp.cos(angles), jnp.sin(angles)))
    return (
        jnp.tile(cos_part, (1, 2 * width // HEAD)),
        jnp.tile(jnp.concatenate([-sin_part, sin_part], axis=1), (1, width // HEAD)),
    )


def swap_halves(values):
    width = values.shape[-1]
    half = HEAD // 2
    if width % 128 == 0:
        lane = lax.broadcasted_iota(jnp.int32, values.shape, 1)
        return jnp.where(
            lane % HEAD < half,
            pltpu.roll(values, width - half, 1),
            pltpu.roll(values, half, 1),
        )
    return jnp.concatenate([values[:, half:], values[:, :half]], axis=-1)


def side_by_side(parts):
    return jnp.concatenate(parts, axis=-1) if len(parts) > 1 else parts[0]


def piece_at(spot_ref, t, piece):
    return pl.ds(pl.multiple_of(spot_ref[t] * piece, piece), piece)


def doc_mask_of(seg_col, seg_row, lo, hi):
    shape = (hi, hi - lo)
    causal = lax.broadcasted_iota(jnp.int32, shape, 0) <= lo + lax.broadcasted_iota(
        jnp.int32, shape, 1
    )
    return (seg_col[:hi] == seg_row[:, lo:hi]) & causal


def attend_forward(
    spot_ref, q_in, k_in, v_in, cos_ref, sin_ref, seg_col, seg_row, q_ref, k_ref, v_ref, att_ref,
    lse_ref, *, piece, blk
):
    rows, width = q_ref.shape
    score_scale = HEAD ** (-0.5)
    for t in range(rows // piece):
        src = piece_at(spot_ref, t, piece)
        dst = slice(t * piece, (t + 1) * piece)
        cos_part, sin_part = cos_ref[dst], sin_ref[dst]
        q_val, k_val = q_in[src].astype(F32), k_in[src].astype(F32)
        q_ref[dst] = (q_val * cos_part + swap_halves(q_val) * sin_part).astype(B16)
        k_ref[dst] = (k_val * cos_part + swap_halves(k_val) * sin_part).astype(B16)
        v_ref[dst] = v_in[src].astype(B16)
    for t in range(rows // blk):
        lo, hi = t * blk, (t + 1) * blk
        mask = doc_mask_of(seg_col, seg_row, lo, hi)
        outs = []
        for h in range(width // HEAD):
            cols = slice(h * HEAD, (h + 1) * HEAD)
            q_blk = q_ref[lo:hi, cols] * B16(score_scale)
            raw = lax.dot_general(k_ref[:hi, cols], q_blk, NT, preferred_element_type=F32)
            raw = jnp.where(mask, raw, NEG_FILL)
            top = jnp.max(raw, axis=0, keepdims=True)
            terms = jnp.exp(raw - top)
            total = jnp.sum(terms, axis=0, keepdims=True)
            probs = (terms * (1.0 / total)).astype(B16)
            outs.append(
                lax.dot_general(probs, v_ref[:hi, cols], TN, preferred_element_type=F32)
            )
            lse_ref[h, :, lo:hi] = jnp.broadcast_to(top + jnp.log(total), (8, blk))
        att = side_by_side(outs).astype(B16)
        for u in range(blk // piece):
            dst = piece_at(spot_ref, t * (blk // piece) + u, piece)
            att_ref[dst] = att[u * piece : (u + 1) * piece]


def attend_backward(
    spot_ref, q_ref, k_ref, v_ref, g_in, lse_ref, cos_ref, sin_ref, seg_col, seg_row, out_ref,
    g_ref, dk_acc, dv_acc, dq_acc, *, piece, blk
):
    rows, width = q_ref.shape
    score_scale = HEAD ** (-0.5)
    for t in range(rows // piece):
        g_ref[t * piece : (t + 1) * piece] = g_in[piece_at(spot_ref, t, piece)]
    for t in reversed(range(rows // blk)):
        lo, hi = t * blk, (t + 1) * blk
        mask = doc_mask_of(seg_col, seg_row, lo, hi)
        dqs, dks, dvs = [], [], []
        for h in range(width // HEAD):
            cols = slice(h * HEAD, (h + 1) * HEAD)
            q_blk, g_blk = q_ref[lo:hi, cols] * B16(score_scale), g_ref[lo:hi, cols]
            raw = lax.dot_general(k_ref[:hi, cols], q_blk, NT, preferred_element_type=F32)
            probs = jnp.exp(jnp.where(mask, raw, NEG_FILL) - lse_ref[h, :1, lo:hi])
            gp = lax.dot_general(v_ref[:hi, cols], g_blk, NT, preferred_element_type=F32)
            inner = jnp.sum(probs * gp, axis=0, keepdims=True)
            gs = (probs * (gp - inner)).astype(B16)
            dvs.append(
                lax.dot_general(probs.astype(B16), g_blk, NN, preferred_element_type=F32)
            )
            dks.append(lax.dot_general(gs, q_blk, NN, preferred_element_type=F32))
            dqs.append(
                lax.dot_general(gs, k_ref[:hi, cols], TN, preferred_element_type=F32)
                * score_scale
            )
        dq_acc[lo:hi] = side_by_side(dqs)
        if hi == rows:
            dk_acc[...] = side_by_side(dks)
            dv_acc[...] = side_by_side(dvs)
        else:
            dk_acc[:hi] += side_by_side(dks)
            dv_acc[:hi] += side_by_side(dvs)
    for t in range(rows // piece):
        dst = piece_at(spot_ref, t, piece)
        src = slice(t * piece, (t + 1) * piece)
        cos_part, sin_part = cos_ref[src], sin_ref[src]
        dq, dk = dq_acc[src], dk_acc[src]
        out_ref[0, dst] = (dq * cos_part - swap_halves(dq) * sin_part).astype(B16)
        out_ref[1, dst] = (dk * cos_part - swap_halves(dk) * sin_part).astype(B16)
        out_ref[2, dst] = dv_acc[src].astype(B16)


def attention_specs(rows, lanes, seq_len):
    width = min(128, lanes)
    return (
        width,
        (lanes // width, rows // seq_len),
        pl.BlockSpec((seq_len, width), lambda i, j, *_: (j, i)),
        pl.BlockSpec((seq_len, width), lambda i, j, *_: (j, 0)),
        pl.BlockSpec((seq_len, 1), lambda i, j, *_: (j, 0)),
        pl.BlockSpec((1, seq_len), lambda i, j, *_: (0, j)),
        pl.BlockSpec((width // HEAD, 8, seq_len), lambda i, j, *_: (i, 0, j)),
    )


def attention(spots, proj, tables, seg_cols, seg_rows, seq_len, piece):
    _, rows, lanes = proj.shape
    width, grid, wide, table, col, row, stat = attention_specs(rows, lanes, seq_len)
    planes = [
        pl.BlockSpec((None, seq_len, width), lambda i, j, *_, n=n: (n, j, i)) for n in range(3)
    ]
    full = jax.ShapeDtypeStruct((rows, lanes), B16)
    return pl.pallas_call(
        functools.partial(attend_forward, piece=piece, blk=min(256, seq_len)),
        out_shape=(full,) * 4 + (jax.ShapeDtypeStruct((lanes // HEAD, 8, rows), F32),),
        grid_spec=pltpu.PrefetchScalarGridSpec(
            num_scalar_prefetch=1,
            grid=grid,
            in_specs=planes + [table, table, col, row],
            out_specs=(wide, wide, wide, wide, stat),
        ),
        compiler_params=PARAMS,
        cost_estimate=TINY,
        name="attend_forward",
    )(spots, proj, proj, proj, *tables, seg_cols, seg_rows)


def attention_back(spots, saved, grad, tables, seg_cols, seg_rows, seq_len, piece):
    q, k, v, lse = saved
    rows, lanes = q.shape
    width, grid, wide, table, col, row, stat = attention_specs(rows, lanes, seq_len)
    return pl.pallas_call(
        functools.partial(attend_backward, piece=piece, blk=min(256, seq_len)),
        out_shape=jax.ShapeDtypeStruct((3, rows, lanes), B16),
        grid_spec=pltpu.PrefetchScalarGridSpec(
            num_scalar_prefetch=1,
            grid=grid,
            in_specs=[wide, wide, wide, wide, stat, table, table, col, row],
            out_specs=pl.BlockSpec((3, seq_len, width), lambda i, j, *_: (0, j, i)),
            scratch_shapes=[pltpu.VMEM((seq_len, width), B16)]
            + [pltpu.VMEM((seq_len, width), F32)] * 3,
        ),
        compiler_params=PARAMS,
        cost_estimate=TINY,
        name="attend_backward",
    )(spots, q, k, v, grad, lse, *tables, seg_cols, seg_rows)


def expand_kernel(x_ref, w_ref, hidden_ref, slope_ref):
    pre = jnp.dot(x_ref[...], w_ref[...], preferred_element_type=F32)
    share = 0.5 * (1.0 + lax.erf(pre * (2.0**-0.5)))
    hidden_ref[...] = (pre * share).astype(B16)
    density = jnp.exp(-0.5 * pre * pre) * ((2.0 * math.pi) ** -0.5)
    slope_ref[...] = (share + pre * density).astype(B16)


def expand(rows_in, weight):
    rows, depth = rows_in.shape
    units = weight.shape[1]
    tile, strip = min(256, units), min(512, rows)
    out = pl.BlockSpec((strip, tile), lambda i, j: (i, j))
    full = jax.ShapeDtypeStruct((rows, units), B16)
    return pl.pallas_call(
        expand_kernel,
        out_shape=(full, full),
        grid=(rows // strip, units // tile),
        in_specs=[
            pl.BlockSpec((strip, depth), lambda i, j: (i, 0)),
            pl.BlockSpec((depth, tile), lambda i, j: (0, j)),
        ],
        out_specs=(out, out),
        compiler_params=PARAMS,
        cost_estimate=TINY,
        name="expand",
    )(rows_in, weight)


def product_kernel(*refs, make, in_count, added, summed):
    acc = make(*refs[:in_count])
    if summed:
        terms = acc * refs[in_count + added][...].astype(F32)
        refs[-1][...] = jnp.sum(terms, axis=0, keepdims=True)
        refs = refs[: in_count + added] + refs[in_count + added + 1 : -1]
    if added:
        acc = acc + refs[in_count][...].astype(F32)
    outs = refs[in_count + added :]
    size = acc.shape[0] // len(outs)
    for i, out_ref in enumerate(outs):
        out_ref[...] = acc[i * size : (i + 1) * size].astype(out_ref.dtype)


def product(name, make, operands, rows, width, got=None, pieces=1, tile=512, against=None):
    strip, tile = min(512, rows), min(tile, width)
    arrays, specs = zip(*[(v, pl.BlockSpec(block, index)) for v, block, index in operands])
    here = lambda i, j: (i, j)
    extra = tuple(v for v in (got, against) if v is not None)
    arrays, specs = arrays + extra, specs + (pl.BlockSpec((strip, tile), here),) * len(extra)
    shapes = [jax.ShapeDtypeStruct((rows // pieces, width), B16)] * pieces
    out_specs = [pl.BlockSpec((strip // pieces, tile), here)] * pieces
    if against is not None:
        shapes.append(jax.ShapeDtypeStruct((rows // strip, 1, width), F32))
        out_specs.append(pl.BlockSpec((None, 1, tile), lambda i, j: (i, 0, j)))
    out = pl.pallas_call(
        functools.partial(
            product_kernel,
            make=make,
            in_count=len(operands),
            added=got is not None,
            summed=against is not None,
        ),
        out_shape=shapes,
        grid=(rows // strip, width // tile),
        in_specs=list(specs),
        out_specs=out_specs,
        compiler_params=SMALL,
        cost_estimate=TINY,
        name=name,
    )(*arrays)
    return list(out)


def times_out(x_ref, w_ref):
    step = x_ref.shape[1]
    return side_by_side(
        [
            jnp.dot(x_ref[...], w_ref[lo : lo + step], preferred_element_type=F32)
            for lo in range(0, w_ref.shape[0], step)
        ]
    )


def times_plain(x_ref, w_ref):
    return jnp.dot(x_ref[...], w_ref[...], preferred_element_type=F32)


def times_turned(x_ref, w_ref):
    return lax.dot_general(x_ref[...], w_ref[...], NT, preferred_element_type=F32)


def times_planes(x_ref, w_ref):
    return sum(
        lax.dot_general(x_ref[n], w_ref[n], NT, preferred_element_type=F32)
        for n in range(x_ref.shape[0])
    )


def scaled_kernel(x_ref, w_ref, slope_ref, out_ref):
    acc = lax.dot_general(x_ref[...], w_ref[...], NT, preferred_element_type=F32)
    out_ref[...] = (slope_ref[...].astype(F32) * acc).astype(B16)


def scaled_product(rows_in, weight, slope):
    rows, depth = rows_in.shape
    units = weight.shape[0]
    tile, strip = min(256, units), min(512, rows)
    here = pl.BlockSpec((strip, tile), lambda i, j: (i, j))
    return pl.pallas_call(
        scaled_kernel,
        out_shape=jax.ShapeDtypeStruct((rows, units), B16),
        grid=(rows // strip, units // tile),
        in_specs=[
            pl.BlockSpec((strip, depth), lambda i, j: (i, 0)),
            pl.BlockSpec((tile, depth), lambda i, j: (j, 0)),
            here,
        ],
        out_specs=here,
        compiler_params=SMALL,
        cost_estimate=TINY,
        name="scaled_product",
    )(rows_in, weight, slope)


def project_kernel(*refs):
    w_ref, out_ref = refs[-2:]
    for n, x_ref in enumerate(refs[:-2]):
        out_ref[n] = jnp.dot(x_ref[...], w_ref[...], preferred_element_type=F32)


def project(parts, four):
    rows, depth = parts[0].shape
    lanes = four.shape[2]
    strip = min(512, rows)
    out = pl.pallas_call(
        project_kernel,
        out_shape=jax.ShapeDtypeStruct((3, len(parts), rows, lanes), F32),
        grid=(rows // strip, 3),
        in_specs=[pl.BlockSpec((strip, depth), lambda i, j: (i, 0)) for _ in parts]
        + [pl.BlockSpec((None, depth, lanes), lambda i, j: (j, 0, 0))],
        out_specs=pl.BlockSpec((None, len(parts), strip, lanes), lambda i, j: (j, 0, i, 0)),
        compiler_params=SMALL,
        cost_estimate=TINY,
        name="project",
    )(*parts, four)
    return out.reshape(3, len(parts) * rows, lanes)


def unmix_kernel(*refs):
    w_ref, out_ref = refs[-2:]
    step = w_ref.shape[1]
    for n, x_ref in enumerate(refs[:-2]):
        acc = None
        for lo in range(0, w_ref.shape[0], step):
            cols = slice(lo, lo + step)
            term = lax.dot_general(x_ref[:, cols], w_ref[cols], NT, preferred_element_type=F32)
            acc = term if acc is None else acc + term
        out_ref[n] = acc.astype(B16)


def unmix(parts, four):
    rows, depth = parts[0].shape
    lanes = four.shape[2]
    strip = min(512, rows)
    out = pl.pallas_call(
        unmix_kernel,
        out_shape=jax.ShapeDtypeStruct((len(parts), rows, lanes), B16),
        grid=(rows // strip,),
        in_specs=[pl.BlockSpec((strip, depth), lambda i: (i, 0)) for _ in parts]
        + [pl.BlockSpec((None, depth, lanes), lambda i: (3, 0, 0))],
        out_specs=pl.BlockSpec((len(parts), strip, lanes), lambda i: (0, i, 0)),
        compiler_params=SMALL,
        cost_estimate=TINY,
        name="unmix",
    )(*parts, four)
    return out.reshape(len(parts) * rows, lanes)


def row_chunks(refs, size):
    return [
        ref.at[slice(lo, lo + size)] for ref in refs for lo in range(0, ref.shape[-2], size)
    ]


def weight_kernel(*refs, x_count, y_count, planes, size, splits, stacked):
    xs, ys, out_ref = refs[:x_count], refs[x_count : x_count + y_count], refs[-1]
    chunks = row_chunks(xs, size)
    for plane in range(planes or 1):
        own = [ref.at[plane] for ref in ys] if planes else ys
        acc = None
        for x_part, y_part in zip(chunks, row_chunks(own, size)):
            term = lax.dot_general(x_part[...], y_part[...], TN, preferred_element_type=F32)
            acc = term if acc is None else acc + term
        acc = acc.astype(B16)
        if planes:
            out_ref[plane] = acc
        elif stacked:
            step = acc.shape[0]
            for n in range(acc.shape[1] // step):
                out_ref[n * step : (n + 1) * step] = acc[:, n * step : (n + 1) * step]
        elif splits:
            step = acc.shape[1] // splits
            for n in range(splits):
                out_ref[n] = acc[:, n * step : (n + 1) * step]
        else:
            out_ref[...] = acc


def weight_grad(
    xs, ys, out_shape, out_block, out_index, x_tile, y_tile, planes=0, splits=0, stacked=False,
    base=None
):
    x_rows, depth = sum(x.shape[0] for x in xs), xs[0].shape[1]
    width = ys[0].shape[-1]
    size = math.gcd(512, *[x.shape[0] for x in xs], *[y.shape[-2] for y in ys])
    x_specs = [pl.BlockSpec((x.shape[0], x_tile), lambda i, j: (0, i)) for x in xs]
    y_specs = [
        pl.BlockSpec((planes, y.shape[1], y_tile), lambda i, j: (0, 0, j))
        if planes
        else pl.BlockSpec((y.shape[0], y_tile), lambda i, j: (0, j))
        for y in ys
    ]
    bases = [] if base is None else [base]
    return pl.pallas_call(
        functools.partial(
            weight_kernel,
            x_count=len(xs),
            y_count=len(ys),
            planes=planes,
            size=size,
            splits=splits,
            stacked=stacked,
        ),
        out_shape=jax.ShapeDtypeStruct(out_shape, B16),
        grid=(depth // x_tile, width // y_tile),
        in_specs=x_specs + y_specs + [pl.BlockSpec(memory_space=pl.ANY) for _ in bases],
        out_specs=pl.BlockSpec(out_block, out_index),
        input_output_aliases={len(xs) + len(ys): 0} if bases else {},
        compiler_params=PARAMS,
        cost_estimate=TINY,
        name="weight_grad",
    )(*xs, *ys, *bases)


def flip(values, bits):
    count = lax.axis_size("col")
    return lax.ppermute(values, "col", [(i, i ^ bits) for i in range(count)])


def send_out(values, direct):
    if not direct:
        return [lax.all_gather(values, "col", axis=0, tiled=True)]
    chips = lax.axis_size("col") // 2
    return [values] + [flip(values, 2 * c) for c in range(1, chips)]


def join(pieces, direct):
    near = jnp.concatenate(pieces, axis=0)
    return [near, flip(near, 1)] if direct else [near]


def spread(values, direct):
    return join(send_out(values, direct), direct)


def near_sum(make, direct, gate=(), later=()):
    if not direct:
        return make(0, None, 1)
    got = flip(after(make(1, None, 1)[0], gate), 1)
    return make(0, after(got, later), lax.axis_size("col") // 2)


def send_sum(near, direct):
    if not direct:
        return [lax.psum_scatter(near[0], "col", scatter_dimension=0, tiled=True)]
    return near[:1] + [flip(v, 2 * c) for c, v in enumerate(near) if c > 0]


def send_both(near, values, direct):
    if not direct:
        return send_sum(near, direct) + send_out(values, direct)
    pairs = [jnp.concatenate([v, w], axis=0) for v, w in zip(near, values)]
    return pairs[:1] + [flip(v, 2 * c) for c, v in enumerate(pairs) if c > 0]


def first_half(pairs, direct):
    return [v[: v.shape[0] // 2] for v in pairs] if direct else pairs[:1]


def last_half(pairs, direct):
    return [v[v.shape[0] // 2 :] for v in pairs] if direct else pairs[1:]


def add_up(parts):
    return sum(v.astype(F32) for v in parts)


def after(values, *others):
    return lax.optimization_barrier((values, others))[0]


def row_shift(values, step):
    count = lax.axis_size("row")
    return lax.ppermute(values, "row", [(i, (i + step) % count) for i in range(count)])


def body(
    layer_in,
    earlier_outs,
    cotangent,
    segments,
    positions,
    w_qkv,
    w_out,
    w_up,
    w_down,
    ln_gains,
    ln_biases,
    dwa_weights,
):
    micro_count, tok_dev, model_width = layer_in.shape
    prior_count = earlier_outs.shape[0]
    col_count = lax.axis_size("col")
    row_count = lax.axis_size("row")
    row_me, col_me = lax.axis_index("row"), lax.axis_index("col")
    direct = col_count == 8
    seq_len = max(SEQ_MIN, SEQ_DEV * col_count)
    group_rows = tok_dev * col_count
    lanes = w_qkv.shape[2]
    part_width = model_width // row_count
    units = w_up.shape[1]
    micros = range(micro_count)

    piece_ids = jnp.arange(col_count, dtype=jnp.int32)
    if direct:
        code = piece_ids ^ col_me
        spots = (code & 1) * (col_count // 2) + (code >> 1)
    else:
        spots = piece_ids

    packed = jnp.concatenate([ln_gains, ln_biases], axis=0)
    norm_params = jnp.zeros((row_count,) + packed.shape, B16)
    norm_params = lax.dynamic_update_index_in_dim(norm_params, packed, row_me, 0)
    for step in range(1, row_count):
        norm_params = lax.dynamic_update_index_in_dim(
            norm_params, row_shift(packed, step), (row_me - step) % row_count, 0
        )
    norm_params = jnp.moveaxis(norm_params, 0, 1).reshape(4, model_width).astype(F32)
    ln_gain, ln_bias = norm_params[:2], norm_params[2:]

    pieces = part_width // lanes
    w_out = jnp.moveaxis(w_out.reshape(lanes, pieces, lanes), 1, 0).reshape(part_width, lanes)
    four_full = lax.all_gather(
        jnp.concatenate([w_qkv, w_out[None]], axis=0), "row", axis=1, tiled=True
    )
    up_full = lax.all_gather(w_up, "row", axis=0, tiled=True)
    down_full = lax.all_gather(w_down, "row", axis=1, tiled=True)

    tables = [rotary_tables(positions[m], min(128, lanes)) for m in micros]
    seg_cols = [segments[m][:, None] for m in micros]
    seg_rows = [segments[m][None, :] for m in micros]

    resid_in = [layer_in[m].astype(F32) for m in micros]
    first = [normalize(v) for v in resid_in]
    normed1 = [(s * ln_gain[0] + ln_bias[0]).astype(B16) for s, _ in first]
    grad_y = [cotangent[m].astype(F32) for m in micros]
    grad_block = [dwa_weights[prior_count] * g for g in grad_y]
    one_pieces, branch_pieces, last = [], [], []
    for m in micros:
        branch_pieces.append(send_out(after(grad_block[m].astype(B16), last), direct))
        one_pieces.append(send_out(after(normed1[m], branch_pieces[m]), direct))
        last = one_pieces[m]
    grad_rows = [join(v, direct) for v in branch_pieces]
    rows_one = [join(after(one_pieces[0], branch_pieces[-1]), direct)]
    rows_one += [join(v, direct) for v in one_pieces[1:]]
    part_rows = group_rows // (2 if direct else 1)
    strip, d_tile = min(512, part_rows), min(512, model_width)
    strips = part_rows // strip

    saved, attended, resid, second, rows_two = [], [], [], [], []
    mixed, mixed_parts, two_pieces = [], [], []

    def norm_two(m, gate):
        resid.append(resid_in[m] + add_up(after(mixed_parts[m], gate)))
        second.append(normalize(resid[m]))
        normed2 = (second[m][0] * ln_gain[1] + ln_bias[1]).astype(B16)
        two_pieces.append(send_out(normed2, direct))
        return normed2

    last = []
    for m in micros:
        proj = project(rows_one[m], after(four_full, mixed[-1]) if m else four_full)
        q, k, v, att, lse = attention(
            spots, proj, tables[m], seg_cols[m], seg_rows[m], seq_len, tok_dev
        )
        saved.append((q, k, v, lse))
        attended.append(att)
        if m > 0:
            last = norm_two(m - 1, att)
        att_m = after(att, last)
        mixed.append(
            near_sum(
                lambda n, got, pieces: product(
                    "mix",
                    times_out,
                    [
                        (att_m, (strip, lanes), lambda i, j: (i + n * strips, 0)),
                        (four_full, (None, d_tile, lanes), lambda i, j: (3, j, 0)),
                    ],
                    part_rows,
                    model_width,
                    got,
                    pieces,
                ),
                direct,
            )
        )
        mixed_parts.append(send_sum(mixed[-1], direct))
    norm_two(micro_count - 1, (two_pieces[-1], up_full))

    flat = lambda lists: [v for parts_of in lists for v in parts_of]
    total_rows = micro_count * group_rows
    fit = max(128, (8 << 20) // (2 * total_rows))
    hidden, slopes, rows_two = [], [], []
    for m in micros:
        rows_two.append(join(after(two_pieces[m], hidden), direct))
        pairs = [expand(v, up_full) for v in rows_two[m]]
        hidden.append([a for a, _ in pairs])
        slopes.append([a for _, a in pairs])
    x_tile, y_tile = min(256, units), min(model_width, fit)
    splits = y_tile // part_width if y_tile > part_width else 0
    y_blocks = part_width // y_tile if y_tile < part_width else 1
    grad_down = weight_grad(
        flat(hidden),
        flat(grad_rows),
        (row_count, units, part_width),
        (splits, x_tile, part_width) if splits else (None, x_tile, y_tile),
        (lambda i, j: (j, i, 0)) if splits else (lambda i, j: (j // y_blocks, i, j % y_blocks)),
        x_tile,
        y_tile,
        splits=splits,
    )
    down_full = after(down_full, grad_down)
    grad_down = lax.psum_scatter(grad_down, "row", scatter_dimension=0, tiled=True)

    grad_pre, back_two, back_parts = [], [], []
    for m in micros:
        slopes_m = after(slopes[m], back_two[-1:])
        grad_pre.append(
            [scaled_product(g, down_full, slope) for slope, g in zip(slopes_m, grad_rows[m])]
        )
        back_two.append(
            near_sum(
                lambda n, got, pieces: product(
                    "unexpand",
                    times_turned,
                    [
                        (grad_pre[m][n], (strip, units), lambda i, j: (i, 0)),
                        (up_full, (d_tile, units), lambda i, j: (j, 0)),
                    ],
                    part_rows,
                    model_width,
                    got,
                    pieces,
                ),
                direct,
                back_parts,
            )
        )
        if m == 0:
            back_parts.append(send_sum(back_two[m], direct))
    grad_normed2, grad_resid, mixed_pieces, branch = [], [], [], []

    shares = []

    def branch_half(m, n, ready, got=None, pieces=1):
        *outs, share = product(
            "contract",
            times_plain,
            [
                (after(hidden[m][n], ready), (strip, units), lambda i, j: (i, 0)),
                (down_full, (units, d_tile), lambda i, j: (0, j)),
            ],
            part_rows,
            model_width,
            got,
            pieces,
            against=grad_rows[m][n],
        )
        shares.append(jnp.sum(share))
        return outs

    x_tile, y_tile = min(256, model_width), min(units, fit)
    def norm_two_back(m, parts):
        grad_normed2.append(add_up(parts))
        grad_resid.append(grad_block[m] + norm_back(grad_normed2[m], *second[m], ln_gain[1]))
        return grad_resid[m].astype(B16)

    chips = col_count // 2 if direct else 1
    grad_mixed = norm_two_back(0, back_parts[0])
    pairs = send_both(back_two[1], [grad_mixed] * chips if direct else grad_mixed, direct)
    grad_up = weight_grad(
        flat(rows_two),
        after(flat(grad_pre), (grad_mixed, back_two[1])),
        (model_width, units),
        (x_tile, y_tile),
        lambda i, j: (i, j),
        x_tile,
        y_tile,
    )
    others = [branch_half(m, 1, grad_up)[0] for m in micros] if direct else [None] * micro_count
    pairs = after(pairs, (grad_up, others if direct else ()))
    grad_up = lax.psum_scatter(grad_up, "row", scatter_dimension=0, tiled=True)
    mixed_pieces.append(last_half(pairs, direct))
    mixed_pieces.append(send_out(norm_two_back(1, first_half(pairs, direct)), direct))
    if direct:
        others = [flip(v, 1) for v in after(others, pairs)]

    grad_planes, grad_mixed_rows = [], []
    for m in micros:
        ready = ()
        if m == 1:
            branch = [branch_half(n, 0, grad_planes[0], others[n], chips) for n in micros]
            if direct:
                branch_pairs = send_both(*branch, direct)
            else:
                branch_pairs = [v for near in branch for v in send_sum(near, direct)]
            ready = (branch, grad_planes[0], grad_down)
        grad_mixed_rows.append(join(after(mixed_pieces[m], ready), direct))
        grad_att = unmix(grad_mixed_rows[m], four_full)
        grad_planes.append(
            attention_back(
                spots, saved[m], grad_att, tables[m], seg_cols[m], seg_rows[m], seq_len, tok_dev
            )
        )

    def back_sum(planes_m, gate, later):
        return near_sum(
            lambda n, got, pieces: product(
                "unproject",
                times_planes,
                [
                    (planes_m, (3, strip, lanes), lambda i, j: (0, i + n * strips, 0)),
                    (four_full, (3, d_tile, lanes), lambda i, j: (0, j, 0)),
                ],
                part_rows,
                model_width,
                got,
                pieces,
            ),
            direct,
            gate,
            later,
        )

    four_shape = (row_count, 4, part_width, lanes)
    grad_four = weight_grad(
        attended,
        flat(grad_mixed_rows),
        four_shape,
        (None, None, part_width, lanes),
        lambda i, j: (j, 3, 0, 0),
        lanes,
        part_width,
        stacked=True,
    )
    x_tile = min(256, part_width)
    per_block = part_width // x_tile
    grad_four = weight_grad(
        flat(rows_one),
        grad_planes,
        four_shape,
        (None, 3, x_tile, lanes),
        lambda i, j: (i // per_block, 0, i % per_block, 0),
        x_tile,
        lanes,
        planes=3,
        base=after(grad_four, grad_up),
    )
    last = grad_four
    grad_four = lax.psum_scatter(grad_four, "row", scatter_dimension=0)

    back_one = [back_sum(after(v, (last, branch_pairs)), (), ()) for v in grad_planes]
    one_parts = [send_sum(v, direct) for v in back_one]
    branch_pairs, cotangent, earlier_outs, grad_down, grad_up = after(
        (branch_pairs, cotangent, earlier_outs, grad_down, grad_up), back_one[-1]
    )
    branch_parts = [first_half(branch_pairs, direct), last_half(branch_pairs, direct)]

    outputs, mix_grads = [], []
    for m in micros:
        block_out = resid[m] + add_up(branch_parts[m])
        earlier = earlier_outs[:, m].astype(F32)
        mix_sum = dwa_weights[0] * earlier[0]
        for level in range(1, prior_count):
            mix_sum = mix_sum + dwa_weights[level] * earlier[level]
        outputs.append((mix_sum + dwa_weights[prior_count] * block_out).astype(B16))
        mix_grads.append(
            jnp.concatenate(
                [
                    jnp.sum(grad_y[m][None] * earlier, axis=(1, 2)),
                    jnp.sum(grad_y[m] * resid[m])[None],
                ]
            )
        )

    grad_earlier = (
        dwa_weights[:prior_count, None, None, None] * cotangent.astype(F32)[None]
    )
    in_grads, grad_normed1 = [], []
    for m in micros:
        grad_normed1.append(add_up(after(one_parts[m], grad_earlier if m else ())))
        in_grads.append(grad_resid[m] + norm_back(grad_normed1[m], *first[m], ln_gain[0]))

    stats = jnp.stack(
        [
            sum(jnp.sum(grad_normed1[m] * first[m][0], axis=0) for m in micros),
            sum(jnp.sum(grad_normed2[m] * second[m][0], axis=0) for m in micros),
            sum(jnp.sum(grad_normed1[m], axis=0) for m in micros),
            sum(jnp.sum(grad_normed2[m], axis=0) for m in micros),
        ]
    )
    mix_sum = sum(mix_grads).at[prior_count].add(sum(shares) / dwa_weights[prior_count])
    mix_row = jnp.pad(mix_sum, (0, part_width - prior_count - 1))
    slabs = jnp.concatenate(
        [
            jnp.moveaxis(stats.reshape(4, row_count, part_width), 1, 0),
            jnp.broadcast_to(mix_row, (row_count, 4, part_width)),
        ],
        axis=1,
    )
    slab = lax.dynamic_index_in_dim(slabs, row_me, 0, keepdims=False)
    for step in range(1, row_count):
        leaving = lax.dynamic_index_in_dim(slabs, (row_me + step) % row_count, 0, keepdims=False)
        slab = slab + row_shift(leaving, step)
    bits = 1
    while bits < col_count:
        slab = slab + flip(slab, bits)
        bits *= 2

    return (
        jnp.stack(outputs),
        jnp.stack(in_grads),
        grad_earlier,
        grad_four[:3].astype(F32),
        jnp.moveaxis(grad_four[3].reshape(pieces, lanes, lanes), 0, 1)
        .reshape(lanes, part_width)
        .astype(F32),
        grad_up.astype(F32),
        grad_down[0].astype(F32),
        slab[:2],
        slab[2:4],
        slab[4, : prior_count + 1],
    )


def solution(mesh):
    in_specs = (
        P(None, ("row", "col"), None),
        P(None, None, ("row", "col"), None),
        P(None, ("row", "col"), None),
        P(None, "row"),
        P(None, "row"),
        P(None, "row", "col"),
        P("col", "row"),
        P("row", "col"),
        P("col", "row"),
        P(None, "row"),
        P(None, "row"),
        P(),
    )
    out_specs = (
        P(None, ("row", "col"), None),
        P(None, ("row", "col"), None),
        P(None, None, ("row", "col"), None),
        P(None, "row", "col"),
        P("col", "row"),
        P("row", "col"),
        P("col", "row"),
        P(None, "row"),
        P(None, "row"),
        P(),
    )
    return jax.shard_map(body, mesh=mesh, in_specs=in_specs, out_specs=out_specs, check_vma=False)
```

```python
import functools
import math

import jax
import jax.numpy as jnp
from jax import lax
from jax.experimental import pallas as pl
from jax.experimental.pallas import tpu as pltpu
from jax.sharding import PartitionSpec as P

HEAD = 64
SEQ_MIN = 1024
SEQ_DEV = 64
EPSILON = 1e-05
NEG_FILL = -1e30
F32 = jnp.float32
B16 = jnp.bfloat16
NT = (((1,), (1,)), ((), ()))
NN = (((1,), (0,)), ((), ()))
TN = (((0,), (0,)), ((), ()))
PARAMS = pltpu.CompilerParams(vmem_limit_bytes=48 << 20)
SMALL = pltpu.CompilerParams(vmem_limit_bytes=24 << 20)
TINY = pl.CostEstimate(flops=1000, bytes_accessed=1000, transcendentals=0)


def normalize(values):
    centre = values - jnp.mean(values, axis=-1, keepdims=True)
    spread = lax.rsqrt(jnp.mean(centre * centre, axis=-1, keepdims=True) + EPSILON)
    return (centre * spread, spread)


def norm_back(grad_normed, scaled, spread, ln_gain):
    shaped = grad_normed * ln_gain
    return spread * (
        shaped
        - jnp.mean(shaped, axis=-1, keepdims=True)
        - scaled * jnp.mean(shaped * scaled, axis=-1, keepdims=True)
    )


def rotary_tables(places, width):
    half_size = HEAD // 2
    inverse = 10000.0 ** (-(jnp.arange(half_size, dtype=F32) * 2.0) / HEAD)
    angles = places.astype(F32)[:, None] * inverse[None, :]
    cos_part, sin_part = lax.optimization_barrier((jnp.cos(angles), jnp.sin(angles)))
    return (
        jnp.tile(cos_part, (1, 2 * width // HEAD)),
        jnp.tile(jnp.concatenate([-sin_part, sin_part], axis=1), (1, width // HEAD)),
    )


def swap_halves(values):
    width = values.shape[-1]
    half = HEAD // 2
    if width % 128 == 0:
        lane = lax.broadcasted_iota(jnp.int32, values.shape, 1)
        return jnp.where(
            lane % HEAD < half,
            pltpu.roll(values, width - half, 1),
            pltpu.roll(values, half, 1),
        )
    return jnp.concatenate([values[:, half:], values[:, :half]], axis=-1)


def side_by_side(parts):
    return jnp.concatenate(parts, axis=-1) if len(parts) > 1 else parts[0]


def piece_at(spot_ref, t, piece):
    return pl.ds(pl.multiple_of(spot_ref[t] * piece, piece), piece)


def doc_mask_of(seg_col, seg_row, lo, hi):
    shape = (hi, hi - lo)
    causal = lax.broadcasted_iota(jnp.int32, shape, 0) <= lo + lax.broadcasted_iota(
        jnp.int32, shape, 1
    )
    return (seg_col[:hi] == seg_row[:, lo:hi]) & causal


def attend_forward(
    spot_ref, q_in, k_in, v_in, cos_ref, sin_ref, seg_col, seg_row, q_ref, k_ref, v_ref, att_ref,
    lse_ref, *, piece, blk
):
    rows, width = q_ref.shape
    score_scale = HEAD ** (-0.5)
    for t in range(rows // piece):
        src = piece_at(spot_ref, t, piece)
        dst = slice(t * piece, (t + 1) * piece)
        cos_part, sin_part = cos_ref[dst], sin_ref[dst]
        q_val, k_val = q_in[src].astype(F32), k_in[src].astype(F32)
        q_ref[dst] = (q_val * cos_part + swap_halves(q_val) * sin_part).astype(B16)
        k_ref[dst] = (k_val * cos_part + swap_halves(k_val) * sin_part).astype(B16)
        v_ref[dst] = v_in[src].astype(B16)
    for t in range(rows // blk):
        lo, hi = t * blk, (t + 1) * blk
        mask = doc_mask_of(seg_col, seg_row, lo, hi)
        outs = []
        for h in range(width // HEAD):
            cols = slice(h * HEAD, (h + 1) * HEAD)
            q_blk = q_ref[lo:hi, cols] * B16(score_scale)
            raw = lax.dot_general(k_ref[:hi, cols], q_blk, NT, preferred_element_type=F32)
            raw = jnp.where(mask, raw, NEG_FILL)
            top = jnp.max(raw, axis=0, keepdims=True)
            terms = jnp.exp(raw - top)
            total = jnp.sum(terms, axis=0, keepdims=True)
            probs = (terms * (1.0 / total)).astype(B16)
            outs.append(
                lax.dot_general(probs, v_ref[:hi, cols], TN, preferred_element_type=F32)
            )
            lse_ref[h, :, lo:hi] = jnp.broadcast_to(top + jnp.log(total), (8, blk))
        att = side_by_side(outs).astype(B16)
        for u in range(blk // piece):
            dst = piece_at(spot_ref, t * (blk // piece) + u, piece)
            att_ref[dst] = att[u * piece : (u + 1) * piece]


def attend_backward(
    spot_ref, q_ref, k_ref, v_ref, g_in, lse_ref, cos_ref, sin_ref, seg_col, seg_row, out_ref,
    g_ref, dk_acc, dv_acc, dq_acc, *, piece, blk
):
    rows, width = q_ref.shape
    score_scale = HEAD ** (-0.5)
    for t in range(rows // piece):
        g_ref[t * piece : (t + 1) * piece] = g_in[piece_at(spot_ref, t, piece)]
    for t in reversed(range(rows // blk)):
        lo, hi = t * blk, (t + 1) * blk
        mask = doc_mask_of(seg_col, seg_row, lo, hi)
        dqs, dks, dvs = [], [], []
        for h in range(width // HEAD):
            cols = slice(h * HEAD, (h + 1) * HEAD)
            q_blk, g_blk = q_ref[lo:hi, cols] * B16(score_scale), g_ref[lo:hi, cols]
            raw = lax.dot_general(k_ref[:hi, cols], q_blk, NT, preferred_element_type=F32)
            probs = jnp.exp(jnp.where(mask, raw, NEG_FILL) - lse_ref[h, :1, lo:hi])
            gp = lax.dot_general(v_ref[:hi, cols], g_blk, NT, preferred_element_type=F32)
            inner = jnp.sum(probs * gp, axis=0, keepdims=True)
            gs = (probs * (gp - inner)).astype(B16)
            dvs.append(
                lax.dot_general(probs.astype(B16), g_blk, NN, preferred_element_type=F32)
            )
            dks.append(lax.dot_general(gs, q_blk, NN, preferred_element_type=F32))
            dqs.append(
                lax.dot_general(gs, k_ref[:hi, cols], TN, preferred_element_type=F32)
                * score_scale
            )
        dq_acc[lo:hi] = side_by_side(dqs)
        if hi == rows:
            dk_acc[...] = side_by_side(dks)
            dv_acc[...] = side_by_side(dvs)
        else:
            dk_acc[:hi] += side_by_side(dks)
            dv_acc[:hi] += side_by_side(dvs)
    for t in range(rows // piece):
        dst = piece_at(spot_ref, t, piece)
        src = slice(t * piece, (t + 1) * piece)
        cos_part, sin_part = cos_ref[src], sin_ref[src]
        dq, dk = dq_acc[src], dk_acc[src]
        out_ref[0, dst] = (dq * cos_part - swap_halves(dq) * sin_part).astype(B16)
        out_ref[1, dst] = (dk * cos_part - swap_halves(dk) * sin_part).astype(B16)
        out_ref[2, dst] = dv_acc[src].astype(B16)


def attention_specs(rows, lanes, seq_len):
    width = min(128, lanes)
    return (
        width,
        (lanes // width, rows // seq_len),
        pl.BlockSpec((seq_len, width), lambda i, j, *_: (j, i)),
        pl.BlockSpec((seq_len, width), lambda i, j, *_: (j, 0)),
        pl.BlockSpec((seq_len, 1), lambda i, j, *_: (j, 0)),
        pl.BlockSpec((1, seq_len), lambda i, j, *_: (0, j)),
        pl.BlockSpec((width // HEAD, 8, seq_len), lambda i, j, *_: (i, 0, j)),
    )


def attention(spots, proj, tables, seg_cols, seg_rows, seq_len, piece):
    _, rows, lanes = proj.shape
    width, grid, wide, table, col, row, stat = attention_specs(rows, lanes, seq_len)
    planes = [
        pl.BlockSpec((None, seq_len, width), lambda i, j, *_, n=n: (n, j, i)) for n in range(3)
    ]
    full = jax.ShapeDtypeStruct((rows, lanes), B16)
    return pl.pallas_call(
        functools.partial(attend_forward, piece=piece, blk=min(256, seq_len)),
        out_shape=(full,) * 4 + (jax.ShapeDtypeStruct((lanes // HEAD, 8, rows), F32),),
        grid_spec=pltpu.PrefetchScalarGridSpec(
            num_scalar_prefetch=1,
            grid=grid,
            in_specs=planes + [table, table, col, row],
            out_specs=(wide, wide, wide, wide, stat),
        ),
        compiler_params=PARAMS,
        cost_estimate=TINY,
        name="attend_forward",
    )(spots, proj, proj, proj, *tables, seg_cols, seg_rows)


def attention_back(spots, saved, grad, tables, seg_cols, seg_rows, seq_len, piece):
    q, k, v, lse = saved
    rows, lanes = q.shape
    width, grid, wide, table, col, row, stat = attention_specs(rows, lanes, seq_len)
    return pl.pallas_call(
        functools.partial(attend_backward, piece=piece, blk=min(256, seq_len)),
        out_shape=jax.ShapeDtypeStruct((3, rows, lanes), B16),
        grid_spec=pltpu.PrefetchScalarGridSpec(
            num_scalar_prefetch=1,
            grid=grid,
            in_specs=[wide, wide, wide, wide, stat, table, table, col, row],
            out_specs=pl.BlockSpec((3, seq_len, width), lambda i, j, *_: (0, j, i)),
            scratch_shapes=[pltpu.VMEM((seq_len, width), B16)]
            + [pltpu.VMEM((seq_len, width), F32)] * 3,
        ),
        compiler_params=PARAMS,
        cost_estimate=TINY,
        name="attend_backward",
    )(spots, q, k, v, grad, lse, *tables, seg_cols, seg_rows)


def expand_kernel(x_ref, w_ref, hidden_ref, slope_ref):
    pre = jnp.dot(x_ref[...], w_ref[...], preferred_element_type=F32)
    share = 0.5 * (1.0 + lax.erf(pre * (2.0**-0.5)))
    hidden_ref[...] = (pre * share).astype(B16)
    density = jnp.exp(-0.5 * pre * pre) * ((2.0 * math.pi) ** -0.5)
    slope_ref[...] = (share + pre * density).astype(B16)


def expand(rows_in, weight):
    rows, depth = rows_in.shape
    units = weight.shape[1]
    tile, strip = min(256, units), min(512, rows)
    out = pl.BlockSpec((strip, tile), lambda i, j: (i, j))
    full = jax.ShapeDtypeStruct((rows, units), B16)
    return pl.pallas_call(
        expand_kernel,
        out_shape=(full, full),
        grid=(rows // strip, units // tile),
        in_specs=[
            pl.BlockSpec((strip, depth), lambda i, j: (i, 0)),
            pl.BlockSpec((depth, tile), lambda i, j: (0, j)),
        ],
        out_specs=(out, out),
        compiler_params=PARAMS,
        cost_estimate=TINY,
        name="expand",
    )(rows_in, weight)


def product_kernel(*refs, make, in_count, added, summed):
    acc = make(*refs[:in_count])
    if summed:
        terms = acc * refs[in_count + added][...].astype(F32)
        refs[-1][...] = jnp.sum(terms, axis=0, keepdims=True)
        refs = refs[: in_count + added] + refs[in_count + added + 1 : -1]
    if added:
        acc = acc + refs[in_count][...].astype(F32)
    outs = refs[in_count + added :]
    size = acc.shape[0] // len(outs)
    for i, out_ref in enumerate(outs):
        out_ref[...] = acc[i * size : (i + 1) * size].astype(out_ref.dtype)


def product(name, make, operands, rows, width, got=None, pieces=1, tile=512, against=None):
    strip, tile = min(512, rows), min(tile, width)
    arrays, specs = zip(*[(v, pl.BlockSpec(block, index)) for v, block, index in operands])
    here = lambda i, j: (i, j)
    extra = tuple(v for v in (got, against) if v is not None)
    arrays, specs = arrays + extra, specs + (pl.BlockSpec((strip, tile), here),) * len(extra)
    shapes = [jax.ShapeDtypeStruct((rows // pieces, width), B16)] * pieces
    out_specs = [pl.BlockSpec((strip // pieces, tile), here)] * pieces
    if against is not None:
        shapes.append(jax.ShapeDtypeStruct((rows // strip, 1, width), F32))
        out_specs.append(pl.BlockSpec((None, 1, tile), lambda i, j: (i, 0, j)))
    out = pl.pallas_call(
        functools.partial(
            product_kernel,
            make=make,
            in_count=len(operands),
            added=got is not None,
            summed=against is not None,
        ),
        out_shape=shapes,
        grid=(rows // strip, width // tile),
        in_specs=list(specs),
        out_specs=out_specs,
        compiler_params=SMALL,
        cost_estimate=TINY,
        name=name,
    )(*arrays)
    return list(out)


def times_out(x_ref, w_ref):
    step = x_ref.shape[1]
    return side_by_side(
        [
            jnp.dot(x_ref[...], w_ref[lo : lo + step], preferred_element_type=F32)
            for lo in range(0, w_ref.shape[0], step)
        ]
    )


def times_plain(x_ref, w_ref):
    return jnp.dot(x_ref[...], w_ref[...], preferred_element_type=F32)


def times_turned(x_ref, w_ref):
    return lax.dot_general(x_ref[...], w_ref[...], NT, preferred_element_type=F32)


def times_planes(x_ref, w_ref):
    return sum(
        lax.dot_general(x_ref[n], w_ref[n], NT, preferred_element_type=F32)
        for n in range(x_ref.shape[0])
    )


def scaled_kernel(x_ref, w_ref, slope_ref, out_ref):
    acc = lax.dot_general(x_ref[...], w_ref[...], NT, preferred_element_type=F32)
    out_ref[...] = (slope_ref[...].astype(F32) * acc).astype(B16)


def scaled_product(rows_in, weight, slope):
    rows, depth = rows_in.shape
    units = weight.shape[0]
    tile, strip = min(256, units), min(512, rows)
    here = pl.BlockSpec((strip, tile), lambda i, j: (i, j))
    return pl.pallas_call(
        scaled_kernel,
        out_shape=jax.ShapeDtypeStruct((rows, units), B16),
        grid=(rows // strip, units // tile),
        in_specs=[
            pl.BlockSpec((strip, depth), lambda i, j: (i, 0)),
            pl.BlockSpec((tile, depth), lambda i, j: (j, 0)),
            here,
        ],
        out_specs=here,
        compiler_params=SMALL,
        cost_estimate=TINY,
        name="scaled_product",
    )(rows_in, weight, slope)


def project_kernel(*refs):
    w_ref, out_ref = refs[-2:]
    for n, x_ref in enumerate(refs[:-2]):
        out_ref[n] = jnp.dot(x_ref[...], w_ref[...], preferred_element_type=F32)


def project(parts, four):
    rows, depth = parts[0].shape
    lanes = four.shape[2]
    strip = min(512, rows)
    out = pl.pallas_call(
        project_kernel,
        out_shape=jax.ShapeDtypeStruct((3, len(parts), rows, lanes), F32),
        grid=(rows // strip, 3),
        in_specs=[pl.BlockSpec((strip, depth), lambda i, j: (i, 0)) for _ in parts]
        + [pl.BlockSpec((None, depth, lanes), lambda i, j: (j, 0, 0))],
        out_specs=pl.BlockSpec((None, len(parts), strip, lanes), lambda i, j: (j, 0, i, 0)),
        compiler_params=SMALL,
        cost_estimate=TINY,
        name="project",
    )(*parts, four)
    return out.reshape(3, len(parts) * rows, lanes)


def unmix_kernel(*refs):
    w_ref, out_ref = refs[-2:]
    step = w_ref.shape[1]
    for n, x_ref in enumerate(refs[:-2]):
        acc = None
        for lo in range(0, w_ref.shape[0], step):
            cols = slice(lo, lo + step)
            term = lax.dot_general(x_ref[:, cols], w_ref[cols], NT, preferred_element_type=F32)
            acc = term if acc is None else acc + term
        out_ref[n] = acc.astype(B16)


def unmix(parts, four):
    rows, depth = parts[0].shape
    lanes = four.shape[2]
    strip = min(512, rows)
    out = pl.pallas_call(
        unmix_kernel,
        out_shape=jax.ShapeDtypeStruct((len(parts), rows, lanes), B16),
        grid=(rows // strip,),
        in_specs=[pl.BlockSpec((strip, depth), lambda i: (i, 0)) for _ in parts]
        + [pl.BlockSpec((None, depth, lanes), lambda i: (3, 0, 0))],
        out_specs=pl.BlockSpec((len(parts), strip, lanes), lambda i: (0, i, 0)),
        compiler_params=SMALL,
        cost_estimate=TINY,
        name="unmix",
    )(*parts, four)
    return out.reshape(len(parts) * rows, lanes)


def row_chunks(refs, size):
    return [
        ref.at[slice(lo, lo + size)] for ref in refs for lo in range(0, ref.shape[-2], size)
    ]


def weight_kernel(*refs, x_count, y_count, planes, size, splits, stacked):
    xs, ys, out_ref = refs[:x_count], refs[x_count : x_count + y_count], refs[-1]
    chunks = row_chunks(xs, size)
    for plane in range(planes or 1):
        own = [ref.at[plane] for ref in ys] if planes else ys
        acc = None
        for x_part, y_part in zip(chunks, row_chunks(own, size)):
            term = lax.dot_general(x_part[...], y_part[...], TN, preferred_element_type=F32)
            acc = term if acc is None else acc + term
        acc = acc.astype(B16)
        if planes:
            out_ref[plane] = acc
        elif stacked:
            step = acc.shape[0]
            for n in range(acc.shape[1] // step):
                out_ref[n * step : (n + 1) * step] = acc[:, n * step : (n + 1) * step]
        elif splits:
            step = acc.shape[1] // splits
            for n in range(splits):
                out_ref[n] = acc[:, n * step : (n + 1) * step]
        else:
            out_ref[...] = acc


def weight_grad(
    xs, ys, out_shape, out_block, out_index, x_tile, y_tile, planes=0, splits=0, stacked=False,
    base=None
):
    x_rows, depth = sum(x.shape[0] for x in xs), xs[0].shape[1]
    width = ys[0].shape[-1]
    size = math.gcd(512, *[x.shape[0] for x in xs], *[y.shape[-2] for y in ys])
    x_specs = [pl.BlockSpec((x.shape[0], x_tile), lambda i, j: (0, i)) for x in xs]
    y_specs = [
        pl.BlockSpec((planes, y.shape[1], y_tile), lambda i, j: (0, 0, j))
        if planes
        else pl.BlockSpec((y.shape[0], y_tile), lambda i, j: (0, j))
        for y in ys
    ]
    bases = [] if base is None else [base]
    return pl.pallas_call(
        functools.partial(
            weight_kernel,
            x_count=len(xs),
            y_count=len(ys),
            planes=planes,
            size=size,
            splits=splits,
            stacked=stacked,
        ),
        out_shape=jax.ShapeDtypeStruct(out_shape, B16),
        grid=(depth // x_tile, width // y_tile),
        in_specs=x_specs + y_specs + [pl.BlockSpec(memory_space=pl.ANY) for _ in bases],
        out_specs=pl.BlockSpec(out_block, out_index),
        input_output_aliases={len(xs) + len(ys): 0} if bases else {},
        compiler_params=PARAMS,
        cost_estimate=TINY,
        name="weight_grad",
    )(*xs, *ys, *bases)


def flip(values, bits):
    count = lax.axis_size("col")
    return lax.ppermute(values, "col", [(i, i ^ bits) for i in range(count)])


def send_out(values, direct):
    if not direct:
        return [lax.all_gather(values, "col", axis=0, tiled=True)]
    chips = lax.axis_size("col") // 2
    return [values] + [flip(values, 2 * c) for c in range(1, chips)]


def join(pieces, direct):
    near = jnp.concatenate(pieces, axis=0)
    return [near, flip(near, 1)] if direct else [near]


def spread(values, direct):
    return join(send_out(values, direct), direct)


def near_sum(make, direct, gate=(), later=()):
    if not direct:
        return make(0, None, 1)
    got = flip(after(make(1, None, 1)[0], gate), 1)
    return make(0, after(got, later), lax.axis_size("col") // 2)


def send_sum(near, direct):
    if not direct:
        return [lax.psum_scatter(near[0], "col", scatter_dimension=0, tiled=True)]
    return near[:1] + [flip(v, 2 * c) for c, v in enumerate(near) if c > 0]


def send_both(near, values, direct):
    if not direct:
        return send_sum(near, direct) + send_out(values, direct)
    pairs = [jnp.concatenate([v, w], axis=0) for v, w in zip(near, values)]
    return pairs[:1] + [flip(v, 2 * c) for c, v in enumerate(pairs) if c > 0]


def first_half(pairs, direct):
    return [v[: v.shape[0] // 2] for v in pairs] if direct else pairs[:1]


def last_half(pairs, direct):
    return [v[v.shape[0] // 2 :] for v in pairs] if direct else pairs[1:]


def add_up(parts):
    return sum(v.astype(F32) for v in parts)


def after(values, *others):
    return lax.optimization_barrier((values, others))[0]


def row_shift(values, step):
    count = lax.axis_size("row")
    return lax.ppermute(values, "row", [(i, (i + step) % count) for i in range(count)])


def body(
    layer_in,
    earlier_outs,
    cotangent,
    segments,
    positions,
    w_qkv,
    w_out,
    w_up,
    w_down,
    ln_gains,
    ln_biases,
    dwa_weights,
):
    micro_count, tok_dev, model_width = layer_in.shape
    prior_count = earlier_outs.shape[0]
    col_count = lax.axis_size("col")
    row_count = lax.axis_size("row")
    row_me, col_me = lax.axis_index("row"), lax.axis_index("col")
    direct = col_count == 8
    seq_len = max(SEQ_MIN, SEQ_DEV * col_count)
    group_rows = tok_dev * col_count
    lanes = w_qkv.shape[2]
    part_width = model_width // row_count
    units = w_up.shape[1]
    micros = range(micro_count)

    piece_ids = jnp.arange(col_count, dtype=jnp.int32)
    if direct:
        code = piece_ids ^ col_me
        spots = (code & 1) * (col_count // 2) + (code >> 1)
    else:
        spots = piece_ids

    packed = jnp.concatenate([ln_gains, ln_biases], axis=0)
    norm_params = jnp.zeros((row_count,) + packed.shape, B16)
    norm_params = lax.dynamic_update_index_in_dim(norm_params, packed, row_me, 0)
    for step in range(1, row_count):
        norm_params = lax.dynamic_update_index_in_dim(
            norm_params, row_shift(packed, step), (row_me - step) % row_count, 0
        )
    norm_params = jnp.moveaxis(norm_params, 0, 1).reshape(4, model_width).astype(F32)
    ln_gain, ln_bias = norm_params[:2], norm_params[2:]

    pieces = part_width // lanes
    w_out = jnp.moveaxis(w_out.reshape(lanes, pieces, lanes), 1, 0).reshape(part_width, lanes)
    four_full = lax.all_gather(
        jnp.concatenate([w_qkv, w_out[None]], axis=0), "row", axis=1, tiled=True
    )
    up_full = lax.all_gather(w_up, "row", axis=0, tiled=True)
    down_full = lax.all_gather(w_down, "row", axis=1, tiled=True)

    tables = [rotary_tables(positions[m], min(128, lanes)) for m in micros]
    seg_cols = [segments[m][:, None] for m in micros]
    seg_rows = [segments[m][None, :] for m in micros]

    resid_in = [layer_in[m].astype(F32) for m in micros]
    first = [normalize(v) for v in resid_in]
    normed1 = [(s * ln_gain[0] + ln_bias[0]).astype(B16) for s, _ in first]
    grad_y = [cotangent[m].astype(F32) for m in micros]
    grad_block = [dwa_weights[prior_count] * g for g in grad_y]
    one_pieces, branch_pieces, last = [], [], []
    for m in micros:
        branch_pieces.append(send_out(after(grad_block[m].astype(B16), last), direct))
        one_pieces.append(send_out(after(normed1[m], branch_pieces[m]), direct))
        last = one_pieces[m]
    grad_rows = [join(v, direct) for v in branch_pieces]
    rows_one = [join(after(one_pieces[0], branch_pieces[-1]), direct)]
    rows_one += [join(v, direct) for v in one_pieces[1:]]
    part_rows = group_rows // (2 if direct else 1)
    strip, d_tile = min(512, part_rows), min(512, model_width)
    strips = part_rows // strip

    saved, attended, resid, second, rows_two = [], [], [], [], []
    mixed, mixed_parts, two_pieces = [], [], []

    def norm_two(m, gate):
        resid.append(resid_in[m] + add_up(after(mixed_parts[m], gate)))
        second.append(normalize(resid[m]))
        normed2 = (second[m][0] * ln_gain[1] + ln_bias[1]).astype(B16)
        two_pieces.append(send_out(normed2, direct))
        return normed2

    last = []
    for m in micros:
        proj = project(rows_one[m], after(four_full, mixed[-1]) if m else four_full)
        q, k, v, att, lse = attention(
            spots, proj, tables[m], seg_cols[m], seg_rows[m], seq_len, tok_dev
        )
        saved.append((q, k, v, lse))
        attended.append(att)
        if m > 0:
            last = norm_two(m - 1, att)
        att_m = after(att, last)
        mixed.append(
            near_sum(
                lambda n, got, pieces: product(
                    "mix",
                    times_out,
                    [
                        (att_m, (strip, lanes), lambda i, j: (i + n * strips, 0)),
                        (four_full, (None, d_tile, lanes), lambda i, j: (3, j, 0)),
                    ],
                    part_rows,
                    model_width,
                    got,
                    pieces,
                ),
                direct,
            )
        )
        mixed_parts.append(send_sum(mixed[-1], direct))
    norm_two(micro_count - 1, (two_pieces[-1], up_full))

    flat = lambda lists: [v for parts_of in lists for v in parts_of]
    total_rows = micro_count * group_rows
    fit = max(128, (8 << 20) // (2 * total_rows))
    hidden, slopes, rows_two = [], [], []
    for m in micros:
        rows_two.append(join(after(two_pieces[m], hidden), direct))
        pairs = [expand(v, up_full) for v in rows_two[m]]
        hidden.append([a for a, _ in pairs])
        slopes.append([a for _, a in pairs])
    x_tile, y_tile = min(256, units), min(model_width, fit)
    splits = y_tile // part_width if y_tile > part_width else 0
    y_blocks = part_width // y_tile if y_tile < part_width else 1
    grad_down = weight_grad(
        flat(hidden),
        flat(grad_rows),
        (row_count, units, part_width),
        (splits, x_tile, part_width) if splits else (None, x_tile, y_tile),
        (lambda i, j: (j, i, 0)) if splits else (lambda i, j: (j // y_blocks, i, j % y_blocks)),
        x_tile,
        y_tile,
        splits=splits,
    )
    down_full = after(down_full, grad_down)
    grad_down = lax.psum_scatter(grad_down, "row", scatter_dimension=0, tiled=True)

    grad_pre, back_two, back_parts = [], [], []
    for m in micros:
        slopes_m = after(slopes[m], back_two[-1:])
        grad_pre.append(
            [scaled_product(g, down_full, slope) for slope, g in zip(slopes_m, grad_rows[m])]
        )
        back_two.append(
            near_sum(
                lambda n, got, pieces: product(
                    "unexpand",
                    times_turned,
                    [
                        (grad_pre[m][n], (strip, units), lambda i, j: (i, 0)),
                        (up_full, (d_tile, units), lambda i, j: (j, 0)),
                    ],
                    part_rows,
                    model_width,
                    got,
                    pieces,
                ),
                direct,
                back_parts,
            )
        )
        if m == 0:
            back_parts.append(send_sum(back_two[m], direct))
    grad_normed2, grad_resid, mixed_pieces, branch = [], [], [], []

    shares = []

    def branch_half(m, n, ready, got=None, pieces=1):
        *outs, share = product(
            "contract",
            times_plain,
            [
                (after(hidden[m][n], ready), (strip, units), lambda i, j: (i, 0)),
                (down_full, (units, d_tile), lambda i, j: (0, j)),
            ],
            part_rows,
            model_width,
            got,
            pieces,
            against=grad_rows[m][n],
        )
        shares.append(jnp.sum(share))
        return outs

    x_tile, y_tile = min(256, model_width), min(units, fit)
    def norm_two_back(m, parts):
        grad_normed2.append(add_up(parts))
        grad_resid.append(grad_block[m] + norm_back(grad_normed2[m], *second[m], ln_gain[1]))
        return grad_resid[m].astype(B16)

    chips = col_count // 2 if direct else 1
    grad_mixed = norm_two_back(0, back_parts[0])
    pairs = send_both(back_two[1], [grad_mixed] * chips if direct else grad_mixed, direct)
    grad_up = weight_grad(
        flat(rows_two),
        after(flat(grad_pre), (grad_mixed, back_two[1])),
        (model_width, units),
        (x_tile, y_tile),
        lambda i, j: (i, j),
        x_tile,
        y_tile,
    )
    others = [branch_half(m, 1, grad_up)[0] for m in micros] if direct else [None] * micro_count
    pairs = after(pairs, (grad_up, others if direct else ()))
    grad_up = lax.psum_scatter(grad_up, "row", scatter_dimension=0, tiled=True)
    mixed_pieces.append(last_half(pairs, direct))
    mixed_pieces.append(send_out(norm_two_back(1, first_half(pairs, direct)), direct))
    if direct:
        others = [flip(v, 1) for v in after(others, pairs)]

    grad_planes, grad_mixed_rows = [], []
    for m in micros:
        ready = ()
        if m == 1:
            branch = [branch_half(n, 0, grad_planes[0], others[n], chips) for n in micros]
            if direct:
                branch_pairs = send_both(*branch, direct)
            else:
                branch_pairs = [v for near in branch for v in send_sum(near, direct)]
            ready = (branch, grad_planes[0], grad_down)
        grad_mixed_rows.append(join(after(mixed_pieces[m], ready), direct))
        grad_att = unmix(grad_mixed_rows[m], four_full)
        grad_planes.append(
            attention_back(
                spots, saved[m], grad_att, tables[m], seg_cols[m], seg_rows[m], seq_len, tok_dev
            )
        )

    def back_sum(planes_m, gate, later):
        return near_sum(
            lambda n, got, pieces: product(
                "unproject",
                times_planes,
                [
                    (planes_m, (3, strip, lanes), lambda i, j: (0, i + n * strips, 0)),
                    (four_full, (3, d_tile, lanes), lambda i, j: (0, j, 0)),
                ],
                part_rows,
                model_width,
                got,
                pieces,
            ),
            direct,
            gate,
            later,
        )

    four_shape = (row_count, 4, part_width, lanes)
    grad_four = weight_grad(
        attended,
        flat(grad_mixed_rows),
        four_shape,
        (None, None, part_width, lanes),
        lambda i, j: (j, 3, 0, 0),
        lanes,
        part_width,
        stacked=True,
    )
    x_tile = min(256, part_width)
    per_block = part_width // x_tile
    grad_four = weight_grad(
        flat(rows_one),
        grad_planes,
        four_shape,
        (None, 3, x_tile, lanes),
        lambda i, j: (i // per_block, 0, i % per_block, 0),
        x_tile,
        lanes,
        planes=3,
        base=grad_four,
    )
    last = grad_four
    grad_four = lax.psum_scatter(grad_four, "row", scatter_dimension=0)

    back_one = [back_sum(after(v, (last, branch_pairs)), (), ()) for v in grad_planes]
    one_parts = [send_sum(v, direct) for v in back_one]
    branch_pairs, cotangent, earlier_outs, grad_down, grad_up = after(
        (branch_pairs, cotangent, earlier_outs, grad_down, grad_up), back_one[-1]
    )
    branch_parts = [first_half(branch_pairs, direct), last_half(branch_pairs, direct)]

    outputs, mix_grads = [], []
    for m in micros:
        block_out = resid[m] + add_up(branch_parts[m])
        earlier = earlier_outs[:, m].astype(F32)
        mix_sum = dwa_weights[0] * earlier[0]
        for level in range(1, prior_count):
            mix_sum = mix_sum + dwa_weights[level] * earlier[level]
        outputs.append((mix_sum + dwa_weights[prior_count] * block_out).astype(B16))
        mix_grads.append(
            jnp.concatenate(
                [
                    jnp.sum(grad_y[m][None] * earlier, axis=(1, 2)),
                    jnp.sum(grad_y[m] * resid[m])[None],
                ]
            )
        )

    grad_earlier = (
        dwa_weights[:prior_count, None, None, None] * cotangent.astype(F32)[None]
    )
    in_grads, grad_normed1 = [], []
    for m in micros:
        grad_normed1.append(add_up(after(one_parts[m], grad_earlier if m else ())))
        in_grads.append(grad_resid[m] + norm_back(grad_normed1[m], *first[m], ln_gain[0]))

    stats = jnp.stack(
        [
            sum(jnp.sum(grad_normed1[m] * first[m][0], axis=0) for m in micros),
            sum(jnp.sum(grad_normed2[m] * second[m][0], axis=0) for m in micros),
            sum(jnp.sum(grad_normed1[m], axis=0) for m in micros),
            sum(jnp.sum(grad_normed2[m], axis=0) for m in micros),
        ]
    )
    mix_sum = sum(mix_grads).at[prior_count].add(sum(shares) / dwa_weights[prior_count])
    mix_row = jnp.pad(mix_sum, (0, part_width - prior_count - 1))
    slabs = jnp.concatenate(
        [
            jnp.moveaxis(stats.reshape(4, row_count, part_width), 1, 0),
            jnp.broadcast_to(mix_row, (row_count, 4, part_width)),
        ],
        axis=1,
    )
    slab = lax.dynamic_index_in_dim(slabs, row_me, 0, keepdims=False)
    for step in range(1, row_count):
        leaving = lax.dynamic_index_in_dim(slabs, (row_me + step) % row_count, 0, keepdims=False)
        slab = slab + row_shift(leaving, step)
    bits = 1
    while bits < col_count:
        slab = slab + flip(slab, bits)
        bits *= 2

    return (
        jnp.stack(outputs),
        jnp.stack(in_grads),
        grad_earlier,
        grad_four[:3].astype(F32),
        jnp.moveaxis(grad_four[3].reshape(pieces, lanes, lanes), 0, 1)
        .reshape(lanes, part_width)
        .astype(F32),
        grad_up.astype(F32),
        grad_down[0].astype(F32),
        slab[:2],
        slab[2:4],
        slab[4, : prior_count + 1],
    )


def solution(mesh):
    in_specs = (
        P(None, ("row", "col"), None),
        P(None, None, ("row", "col"), None),
        P(None, ("row", "col"), None),
        P(None, "row"),
        P(None, "row"),
        P(None, "row", "col"),
        P("col", "row"),
        P("row", "col"),
        P("col", "row"),
        P(None, "row"),
        P(None, "row"),
        P(),
    )
    out_specs = (
        P(None, ("row", "col"), None),
        P(None, ("row", "col"), None),
        P(None, None, ("row", "col"), None),
        P(None, "row", "col"),
        P("col", "row"),
        P("row", "col"),
        P("col", "row"),
        P(None, "row"),
        P(None, "row"),
        P(),
    )
    return jax.shard_map(body, mesh=mesh, in_specs=in_specs, out_specs=out_specs, check_vma=False)
```
